512 devices in a mesh: gy: 32 (over z, y_lo), gz: 16 (over x, y_hi, core).
Axes of the slice: x: 4, y: 8 (y_hi: 2, y_lo: 4; y = y_hi * 4 + y_lo), z: 8, core: 2. Of those that a mesh axis runs over, the one named last changes fastest.
Arguments:
- scalar: float32 [64, 768, 768], P('gz', 'gy'), may hold values from -6 to 6
- velocity: float32 [3, 64, 256, 256], P(None, None, 'gy', 'gz'), may hold values from -0.9 to 0.9
Outputs:
- remeshed: float32 [64, 768, 768], P('gz', 'gy')
The draws below stay inside these ranges and needn't reach their ends.
All inputs are finite; a program needn't handle non-finite values.
Results may differ from the reference program's by a relative error of at most 0.0003.
Values sent between devices are 32-bit elements; how exact they have to be, the bound alone decides.
A program may use at most 64 MiB of HBM per device.

```python
import jax
import jax.numpy as jnp
from jax import lax

NX = 768
NY = 768
NZ = 64
NXC = 256
NYC = 256


def level_of(stream_key, dims, cuts, smallest, high):
    factor_of = 1.0
    for position, shards_of in cuts:
        heights = jax.random.uniform(jax.random.fold_in(jax.random.fold_in(stream_key, 6), position), (shards_of,), jnp.float32, smallest / len(cuts), high / len(cuts))
        factor_of = factor_of * jnp.repeat(jnp.exp(heights), dims[position] // shards_of).reshape((-1,) + (1,) * (len(dims) - 1 - position))
    return factor_of


def bell_draw(stream_key, dims, scale, most, cuts=(), held_as=jnp.bfloat16):
    gain = level_of(stream_key, dims, cuts, -0.22, 0.18) if cuts else 1.0
    array = jax.random.normal(stream_key, dims, jnp.float32) * scale * gain
    return jnp.minimum(jnp.maximum(array, -most), most).astype(held_as)


def setup_inputs(seed: int = 0) -> dict:
    key_of = jax.random.split(jax.random.key(seed), 3)
    scalar = bell_draw(key_of[0], (NZ, NY, NX), 1.0, 6.0, ((0, 16), (1, 32)), jnp.float32)
    velocity = jnp.clip(jax.random.uniform(key_of[1], (3, NZ, NYC, NXC), jnp.float32, -0.9, 0.9) * level_of(key_of[1], (3, NZ, NYC, NXC), ((2, 32), (3, 16)), -0.4, 0.0), -0.9, 0.9)
    return {"scalar": scalar, "velocity": velocity}


def alternate(current, following, along):
    pieces = [current * (1.0 - phase / 3.0) + following * (phase / 3.0) for phase in range(3)]
    stacked = jnp.stack(pieces, axis=along + 1)
    new_shape = list(current.shape)
    new_shape[along] = new_shape[along] * 3
    return stacked.reshape(new_shape)


def polynomial(factors, value):
    result = jnp.zeros_like(value)
    for factor in reversed(factors):
        result = result * value + factor
    return result


def kernel_weight(offset):
    size = jnp.abs(offset)
    inner = polynomial([1.0, 0.0, -5.0 / 4.0, -35.0 / 12.0, 21.0 / 4.0, -25.0 / 12.0], size)
    middle = polynomial([-4.0, 75.0 / 4.0, -245.0 / 8.0, 545.0 / 24.0, -63.0 / 8.0, 25.0 / 24.0], size)
    outer = polynomial([18.0, -153.0 / 4.0, 255.0 / 8.0, -313.0 / 24.0, 21.0 / 8.0, -5.0 / 24.0], size)
    return jnp.where(size < 1.0, inner, jnp.where(size < 2.0, middle, jnp.where(size < 3.0, outer, 0.0)))


def displacement(speed, before, after):
    half_step = 0.5 * speed
    return jnp.where(half_step >= 0.0, (1.0 - half_step) * speed + half_step * after, (1.0 + half_step) * speed - half_step * before)


def sweep_periodic(field, speed, along):
    moved = displacement(speed, jnp.roll(speed, 1, along), jnp.roll(speed, -1, along))
    result = jnp.zeros_like(field)
    for offset in range(-3, 4):
        result = result + jnp.roll(field * kernel_weight(offset - moved), offset, along)
    return result


def sweep_open(field, speed):
    zero_plane = jnp.zeros_like(speed[:1])
    before = jnp.concatenate([zero_plane, speed[:-1]], axis=0)
    after = jnp.concatenate([speed[1:], zero_plane], axis=0)
    moved = displacement(speed, before, after)
    count = field.shape[0]
    total = jnp.zeros((count + 6,) + field.shape[1:], jnp.float32)
    for offset in range(-3, 4):
        total = total.at[3 + offset:3 + offset + count].add(field * kernel_weight(offset - moved))
    return total[3:3 + count]


def plane_sweeps(pair):
    plane, coarse = pair
    y_fine = alternate(coarse, jnp.roll(coarse, -1, 1), 1)
    fine_vel = alternate(y_fine, jnp.roll(y_fine, -1, 2), 2)
    field = sweep_periodic(plane, fine_vel[0], 1)
    field = sweep_periodic(field, fine_vel[1], 0)
    return field.T, fine_vel[2].T


def column_sweep(pair):
    return sweep_open(pair[0], pair[1])


def reference(scalar, velocity):
    swept, vertical = lax.map(plane_sweeps, (scalar, jnp.moveaxis(velocity, 1, 0)))
    columns = lax.map(column_sweep, (jnp.moveaxis(swept, 1, 0), jnp.moveaxis(vertical, 1, 0)))
    return jnp.moveaxis(columns, 0, 1)
```

```python
import functools

import jax
import jax.numpy as jnp
from jax import lax
from jax.experimental import pallas as pl
from jax.experimental.pallas import tpu as pltpu
from jax.sharding import PartitionSpec as P

MESH = pl.DeviceIdType.MESH
F32 = jnp.float32
BF16 = jnp.bfloat16
NGY = 32
NGZ = 16
PLANES = 4
ROWS = 24
NX = 768
LANES = 128
TILES = NX // LANES


def copy_to(src, dst, send, recv, gy, gz):
    return pltpu.make_async_remote_copy(
        src, dst, send, recv, device_id={"gy": gy, "gz": gz}, device_id_type=MESH
    )


def wait_for(ref, sem):
    pltpu.make_async_copy(ref, ref, sem).wait()


def moved_by(speed, before, after):
    half = jnp.abs(0.5 * speed)
    return speed + half * (jnp.where(speed >= 0.0, after, before) - speed)


def products(q, d):
    a = jnp.abs(d)
    b = 1.0 - a
    w = a * b
    p3 = (w * (a * a)) * (7.0 / 24.0 - (5.0 / 24.0) * a)
    pm2 = w * (1.0 / 12.0 + a * (1.0 / 24.0 + a * (-1.0 / 3.0 + (5.0 / 24.0) * a)))
    p2 = w * (-1.0 / 12.0 + a * (-1.0 / 8.0 + a * (-3.0 / 2.0 + (25.0 / 24.0) * a)))
    pm1 = w * (-2.0 / 3.0 + (a * a) * (13.0 / 8.0 - (25.0 / 24.0) * a))
    p1 = a + pm1 + 2.0 * (pm2 - p2) - 3.0 * p3
    p0 = 1.0 - (p1 + pm1) - (p2 + pm2) - p3
    right = d >= 0.0
    q0, q1, qm1, q2, qm2, q3 = (q * p for p in (p0, p1, pm1, p2, pm2, p3))
    return {
        0: q0,
        1: jnp.where(right, q1, qm1),
        -1: jnp.where(right, qm1, q1),
        2: jnp.where(right, q2, qm2),
        -2: jnp.where(right, qm2, q2),
        3: jnp.where(right, q3, 0.0),
        -3: jnp.where(right, 0.0, q3),
    }


def lane_roll(value, amount):
    amount = amount % value.shape[-1]
    return value if amount == 0 else pltpu.roll(value, amount, value.ndim - 1)


def row_roll(value, amount):
    amount = amount % value.shape[0]
    return value if amount == 0 else pltpu.roll(value, amount, 0)


def kernel(
    scalar_ref,
    vel_ref,
    out_ref,
    packed,
    send_v,
    send_n,
    send_p,
    recv_v,
    recv_n,
    recv_p,
    hal_up,
    hal_dn,
    got_up,
    got_dn,
    refine,
    coarse,
    scal,
    fine,
    field,
    edge,
    own,
    cross,
    part,
    recv_d,
    t_own,
    t_cross,
    recv_o,
    recv_c,
    sems,
):
    gy, gz = lax.axis_index("gy"), lax.axis_index("gz")
    odd = gz % 2
    next_y, prev_y = (gy + 1) % NGY, (gy + NGY - 1) % NGY
    partner = gz + 1 - 2 * odd
    other = gz - 1 + 2 * odd
    has_other = jnp.logical_and(other >= 0, other < NGZ)
    n_other = has_other.astype(jnp.int32)
    lane = lax.broadcasted_iota(jnp.int32, (8, LANES), 1)

    barrier = pltpu.get_barrier_semaphore()

    def greet(y, z):
        pl.semaphore_signal(
            barrier, inc=1, device_id={"gy": y, "gz": z}, device_id_type=MESH
        )

    def greet_z(i, _):
        greet(gy, (gz + i) % NGZ)
        return _

    def greet_zn(i, _):
        greet(next_y, (gz + i) % NGZ)
        greet(prev_y, (gz + i) % NGZ)
        return _

    def greet_y(i, _):
        greet((gy + i) % NGY, gz)
        return _

    def greet_o(i, _):
        greet((gy + i) % NGY, other)
        return _

    lax.fori_loop(1, NGZ, greet_z, 0)
    lax.fori_loop(0, NGZ, greet_zn, 0)
    lax.fori_loop(2, NGY - 1, greet_y, 0)

    @pl.when(has_other)
    def _():
        lax.fori_loop(2, NGY - 1, greet_o, 0)

    for group in range(24):
        total = jnp.zeros((8, LANES), F32)
        for y in range(8):
            rows = vel_ref[pl.ds(group * 64 + y, 8, stride=8), :]
            wide = jnp.concatenate([rows, jnp.zeros((8, LANES - 16), F32)], axis=1)
            total = total + lane_roll(wide, 16 * y)
        packed[8 + group * 8 : 16 + group * 8, :] = total
    for z in range(NGZ):
        send_v[z, 0:4, :] = packed[8 + 4 * z : 12 + 4 * z, :]
        send_v[z, 4:8, :] = packed[72 + 4 * z : 76 + 4 * z, :]
        up = packed[135 + 4 * z : 141 + 4 * z, :] if z < NGZ - 1 else packed[135 + 4 * z : 140 + 4 * z, :]
        if z == 0:
            row = lax.broadcasted_iota(jnp.int32, up.shape, 0)
            up = jnp.where(row == 0, 0.0, up)
        if z == NGZ - 1:
            send_v[z, 8:13, :] = up
            send_v[z, 13:14, :] = jnp.zeros((1, LANES), F32)
        else:
            send_v[z, 8:14, :] = up
    lane4 = lax.broadcasted_iota(jnp.int32, (4, LANES), 1)
    for z in range(NGZ):
        first = jnp.zeros((4, LANES), F32)
        last = jnp.zeros((4, LANES), F32)
        for q in range(4):
            if q < 3:
                rows = send_v[z, 4 * q : 4 * q + 4, :]
            else:
                rows = jnp.concatenate(
                    [send_v[z, 12:14, :], jnp.zeros((2, LANES), F32)], axis=0
                )
            here = jnp.logical_and(lane4 >= 32 * q, lane4 < 32 * q + 32)
            first = jnp.where(here, lane_roll(rows, 32 * q), first)
            if q < 2:
                last = jnp.where(here, lane_roll(rows, 32 + 32 * q), last)
        send_n[z] = first
        send_p[z] = last
    for k in range(3):
        for z in range(PLANES):
            hal_up[4 * k + z : 4 * k + z + 1, :] = scalar_ref[z, k : k + 1, :]
            hal_dn[4 * k + z : 4 * k + z + 1, :] = scalar_ref[z, 21 + k : 22 + k, :]
    for z in range(PLANES):
        for t in range(TILES):
            scal[t, ROWS * z : ROWS * z + ROWS, :] = scalar_ref[
                z, :, LANES * t : LANES * t + LANES
            ]
    for block in range(16):
        r = lax.broadcasted_iota(jnp.int32, (16, NX), 0) + 16 * block
        c = lax.broadcasted_iota(jnp.int32, (16, NX), 1)
        t = jnp.abs(c - 3 * r)
        if block == 0:
            t = jnp.where(r == 0, jnp.minimum(t, jnp.abs(c - NX)), t)
        refine[16 * block : 16 * block + 16, :] = (
            jnp.maximum(3 - t, 0).astype(F32).astype(BF16)
        )

    pl.semaphore_wait(barrier, 105 - 29 + 29 * n_other)

    def send_z(i, _):
        z = (gz + i) % NGZ
        copy_to(send_v.at[z], recv_v.at[gz], sems.at[0], sems.at[1], gy, z).start()
        return _

    def send_zn(i, _):
        z = (gz + i) % NGZ
        copy_to(send_n.at[z], recv_n.at[gz], sems.at[2], sems.at[3], prev_y, z).start()
        copy_to(send_p.at[z], recv_p.at[gz], sems.at[4], sems.at[5], next_y, z).start()
        return _

    lax.fori_loop(1, NGZ, send_z, 0)
    lax.fori_loop(0, NGZ, send_zn, 0)
    to_prev = copy_to(hal_up, got_dn, sems.at[6], sems.at[7], prev_y, gz)
    to_next = copy_to(hal_dn, got_up, sems.at[8], sems.at[9], next_y, gz)
    to_prev.start()
    to_next.start()
    recv_v[gz] = send_v[gz]

    wait_for(recv_v.at[0:15], sems.at[1])
    wait_for(recv_n, sems.at[3])
    wait_for(recv_p, sems.at[5])

    for c in range(8):
        for half in range(2):
            top = jnp.zeros((8, LANES), F32)
            low = jnp.zeros((6, LANES), F32)
            for i in range(8):
                g = 8 * half + i
                here = jnp.logical_and(lane >= 16 * i, lane < 16 * i + 16)
                top = jnp.where(here, lane_roll(recv_v[g, 0:8, :], 16 * (i - c)), top)
                low = jnp.where(
                    here[0:6], lane_roll(recv_v[g, 8:14, :], 16 * (i - c)), low
                )
            base = 16 * (c + 2)
            columns = pl.ds(LANES * half, LANES)
            coarse[base : base + 8, columns] = top
            coarse[base + 8 : base + 14, columns] = low
            coarse[base + 14 : base + 16, columns] = jnp.zeros((2, LANES), F32)
    for c in (-2, -1, 8, 9):
        source, offset, chunks = (recv_n, c - 8, 4) if c > 0 else (recv_p, c + 2, 2)
        base = 16 * (c + 2)
        for half in range(2):
            columns = pl.ds(LANES * half, LANES)
            for q in range(4):
                total = jnp.zeros((4, LANES), F32)
                if q < chunks:
                    for i in range(8):
                        here = jnp.logical_and(lane4 >= 16 * i, lane4 < 16 * i + 16)
                        rows = source[8 * half + i]
                        total = jnp.where(
                            here, lane_roll(rows, 16 * i - 32 * q - 16 * offset), total
                        )
                coarse[base + 4 * q : base + 4 * q + 4, columns] = total
    value = coarse[...]
    high = value.astype(BF16)
    low = (value - high.astype(F32)).astype(BF16)
    for pair in range(TILES // 2):
        weights = refine[:, 2 * LANES * pair : 2 * LANES * (pair + 1)]
        result = (
            jnp.dot(high, weights, preferred_element_type=F32)
            + jnp.dot(low, weights, preferred_element_type=F32)
        ) * (1.0 / 3.0)
        fine[2 * pair] = result[:, :LANES]
        fine[2 * pair + 1] = result[:, LANES:]

    def level(first, plane, t):
        return fine[t, pl.ds(16 * (first + 2) + plane, 8, stride=16), :]

    def edge_level(shift, plane, t):
        return jnp.concatenate(
            [
                fine[t, pl.ds(16 * (1 + shift) + plane, 4), :],
                fine[t, pl.ds(16 * (10 + shift) + plane, 4), :],
            ],
            axis=0,
        )

    def whole(load):
        return jnp.concatenate([load(t) for t in range(TILES)], axis=1)

    def spread(ref, rows, value):
        for t in range(TILES):
            ref[t, rows, :] = value[:, LANES * t : LANES * t + LANES]

    def mixed(base, following, k):
        return base if k == 0 else base * (1.0 - k / 3.0) + following * (k / 3.0)

    def sweep_x(q, u):
        d = moved_by(u, lane_roll(u, 1), lane_roll(u, -1))
        terms = products(q, d)
        total = terms[0]
        for m in (-3, -2, -1, 1, 2, 3):
            total = total + lane_roll(terms[m], m)
        return total

    for z in range(PLANES):
        base = whole(functools.partial(level, 0, z))
        following = whole(functools.partial(level, 1, z))
        for k in range(3):
            q = whole(lambda t: scal[t, pl.ds(ROWS * z + k, 8, stride=3), :])
            i = 8 * (3 * z + k)
            spread(field, slice(i, i + 8), sweep_x(q, mixed(base, following, k)))
    wait_for(got_up, sems.at[7])
    wait_for(got_dn, sems.at[9])
    base = whole(functools.partial(edge_level, 0, 0))
    following = whole(functools.partial(edge_level, 1, 0))
    for k in range(3):
        q = jnp.concatenate(
            [got_up[4 * k : 4 * k + 4, :], got_dn[4 * k : 4 * k + 4, :]], axis=0
        )
        spread(
            edge, slice(8 * k, 8 * k + 8), sweep_x(q, mixed(base, following, k))
        )

    row = lax.broadcasted_iota(jnp.int32, (8, LANES), 0)

    def phases(before, base, following, q_of):
        u = [mixed(base, following, k) for k in range(3)]
        sides = [mixed(before, base, 2)] + u + [following]
        sums = {}
        for k in range(3):
            terms = products(q_of(k), moved_by(u[k], sides[k], sides[k + 2]))
            for m in range(-3, 4):
                key = ((k + m) % 3, (k + m) // 3)
                sums[key] = terms[m] if key not in sums else sums[key] + terms[m]
        return sums

    def tile_step(t, _):
        edges = phases(
            edge_level(-1, 4, t),
            edge_level(0, 4, t),
            edge_level(1, 4, t),
            lambda k: edge[t, 8 * k : 8 * k + 8, :],
        )
        swept = {}
        for z in range(PLANES):
            sums = phases(
                level(-1, 4 + z, t),
                level(0, 4 + z, t),
                level(1, 4 + z, t),
                lambda k: field[t, 8 * (3 * z + k) : 8 * (3 * z + k) + 8, :],
            )
            for k in range(3):
                above = jnp.where(
                    row == 0, row_roll(edges[k, 1], -z), row_roll(sums[k, 1], 1)
                )
                below = jnp.where(
                    row == 7, row_roll(edges[k, -1], 3 - z), row_roll(sums[k, -1], -1)
                )
                swept[z, k] = sums[k, 0] + above + below
        lower = [level(0, 8 + p, t) for p in range(6)]
        upper = [level(1, 8 + p, t) for p in range(6)]
        for k in range(3):
            u = [mixed(lower[p], upper[p], k) for p in range(6)]
            sums = {}
            for z in range(PLANES):
                terms = products(swept[z, k], moved_by(u[z + 1], u[z], u[z + 2]))
                for m in range(-3, 4):
                    sums[z + m] = terms[m] if z + m not in sums else sums[z + m] + terms[m]
            for z in range(PLANES):
                own[t, pl.ds(ROWS * z + k, 8, stride=3), :] = sums[z]
            for i in range(3):
                up, down = sums[4 + i], sums[i - 3]
                cross[t, pl.ds(ROWS * i + k, 8, stride=3), :] = jnp.where(
                    odd == 1, up, down
                )
                part[t, pl.ds(ROWS * i + k, 8, stride=3), :] = jnp.where(
                    odd == 1, down, up
                )
        return _

    lax.fori_loop(0, TILES, tile_step, 0)

    to_partner = copy_to(part, recv_d, sems.at[10], sems.at[11], gy, partner)
    to_partner.start()

    def transposed(source, target):
        for t in range(TILES):
            target[LANES * t : LANES * t + LANES, :] = source[t].T

    def dest(i):
        y = (gy + i) % NGY
        return y, pl.ds(pl.multiple_of(ROWS * y, 8), ROWS)

    @pl.when(has_other)
    def _():
        transposed(cross, t_cross)

        def send(i, _):
            y, rows = dest(i)
            copy_to(
                t_cross.at[rows], recv_c.at[gy], sems.at[12], sems.at[13], y, other
            ).start()
            return _

        lax.fori_loop(0, NGY, send, 0)

    wait_for(recv_d, sems.at[11])
    target = pl.ds(pl.multiple_of(ROWS * odd_to_first(odd), 8), 72)
    own[:, target, :] = own[:, target, :] + recv_d[...]
    transposed(own, t_own)

    def send_own(i, _):
        y, rows = dest(i)
        copy_to(t_own.at[rows], recv_o.at[gy], sems.at[14], sems.at[15], y, gz).start()
        return _

    lax.fori_loop(1, NGY, send_own, 0)
    recv_o[gy] = t_own[pl.ds(pl.multiple_of(ROWS * gy, 8), ROWS), :]

    @pl.when(has_other)
    def _():
        wait_for(recv_c, sems.at[13])

    @pl.when(jnp.logical_not(has_other))
    def _():
        recv_c[...] = jnp.zeros_like(recv_c)

    wait_for(recv_o.at[0 : NGY - 1], sems.at[15])

    keep = lane < 3 * ROWS

    for x in range(3):
        rows = pl.ds(8 * x, 8)
        totals = {}
        for y in range(NGY):
            extra = jnp.where(keep, recv_c[y, rows, :], 0.0)
            moved = lane_roll(extra, ROWS)
            value = recv_o[y, rows, :] + jnp.where(odd == 1, moved, extra)
            start = ROWS * y
            for z in range(PLANES):
                turned = lane_roll(value, ROWS * (y - z))
                for t in range(start // LANES, (start + ROWS - 1) // LANES + 1):
                    at = lane + LANES * t
                    here = jnp.logical_and(at >= start, at < start + ROWS)
                    old = totals.get((z, t))
                    totals[z, t] = (
                        turned if old is None else jnp.where(here, turned, old)
                    )
            for t in range(TILES):
                if (t + 1) * LANES <= start + ROWS and (0, t) in totals:
                    for z in range(PLANES):
                        out_ref[z, rows, LANES * t : LANES * t + LANES] = totals.pop(
                            (z, t)
                        )

    wait_for(send_v.at[0:15], sems.at[0])
    wait_for(send_n, sems.at[2])
    wait_for(send_p, sems.at[4])
    wait_for(hal_up, sems.at[6])
    wait_for(hal_dn, sems.at[8])
    wait_for(part, sems.at[10])
    wait_for(recv_o.at[0 : NGY - 1], sems.at[14])

    @pl.when(has_other)
    def _():
        wait_for(recv_c, sems.at[12])


def odd_to_first(odd):
    return 1 - odd


def local(scalar, velocity):
    vmem = pl.BlockSpec(memory_space=pltpu.VMEM)
    buffers = [
        (208, LANES),
        (NGZ, 14, LANES),
        (NGZ, 4, LANES),
        (NGZ, 4, LANES),
        (NGZ, 14, LANES),
        (NGZ, 4, LANES),
        (NGZ, 4, LANES),
        (12, NX),
        (12, NX),
        (12, NX),
        (12, NX),
    ]
    later = [
        (192, 256),
        (TILES, 96, LANES),
        (TILES, 192, LANES),
        (TILES, 96, LANES),
        (TILES, 24, LANES),
        (TILES, LANES, LANES),
        (TILES, LANES, LANES),
        (TILES, 72, LANES),
        (TILES, 72, LANES),
        (NX, LANES),
        (NX, LANES),
        (NGY, ROWS, LANES),
        (NGY, ROWS, LANES),
    ]
    return pl.pallas_call(
        kernel,
        out_shape=jax.ShapeDtypeStruct((PLANES, ROWS, NX), F32),
        in_specs=[vmem, vmem],
        out_specs=vmem,
        scratch_shapes=[pltpu.VMEM(s, F32) for s in buffers]
        + [pltpu.VMEM((256, NX), BF16)]
        + [pltpu.VMEM(s, F32) for s in later]
        + [pltpu.SemaphoreType.DMA((16,))],
        compiler_params=pltpu.CompilerParams(collective_id=0, has_side_effects=True),
    )(scalar, velocity.reshape(3 * 64 * 8, 16))


def solution(mesh):
    in_specs = (P("gz", "gy", None), P(None, None, "gy", "gz"))
    out_specs = P("gz", "gy", None)
    return jax.shard_map(
        local, mesh=mesh, in_specs=in_specs, out_specs=out_specs, check_vma=False
    )
```

```python
import functools

import jax
import jax.numpy as jnp
from jax import lax
from jax.experimental import pallas as pl
from jax.experimental.pallas import tpu as pltpu
from jax.sharding import PartitionSpec as P

MESH = pl.DeviceIdType.MESH
F32 = jnp.float32
BF16 = jnp.bfloat16
NGY = 32
NGZ = 16
PLANES = 4
ROWS = 24
NX = 768
LANES = 128
TILES = NX // LANES


def copy_to(src, dst, send, recv, gy, gz):
    return pltpu.make_async_remote_copy(
        src, dst, send, recv, device_id={"gy": gy, "gz": gz}, device_id_type=MESH
    )


def wait_for(ref, sem):
    pltpu.make_async_copy(ref, ref, sem).wait()


def moved_by(speed, before, after):
    half = jnp.abs(0.5 * speed)
    return speed + half * (jnp.where(speed >= 0.0, after, before) - speed)


def products(q, d):
    a = jnp.abs(d)
    b = 1.0 - a
    w = a * b
    p3 = (w * (a * a)) * (7.0 / 24.0 - (5.0 / 24.0) * a)
    pm2 = w * (1.0 / 12.0 + a * (1.0 / 24.0 + a * (-1.0 / 3.0 + (5.0 / 24.0) * a)))
    p2 = w * (-1.0 / 12.0 + a * (-1.0 / 8.0 + a * (-3.0 / 2.0 + (25.0 / 24.0) * a)))
    pm1 = w * (-2.0 / 3.0 + (a * a) * (13.0 / 8.0 - (25.0 / 24.0) * a))
    p1 = a + pm1 + 2.0 * (pm2 - p2) - 3.0 * p3
    p0 = 1.0 - (p1 + pm1) - (p2 + pm2) - p3
    right = d >= 0.0
    q0, q1, qm1, q2, qm2, q3 = (q * p for p in (p0, p1, pm1, p2, pm2, p3))
    return {
        0: q0,
        1: jnp.where(right, q1, qm1),
        -1: jnp.where(right, qm1, q1),
        2: jnp.where(right, q2, qm2),
        -2: jnp.where(right, qm2, q2),
        3: jnp.where(right, q3, 0.0),
        -3: jnp.where(right, 0.0, q3),
    }


def lane_roll(value, amount):
    amount = amount % value.shape[-1]
    return value if amount == 0 else pltpu.roll(value, amount, value.ndim - 1)


def row_roll(value, amount):
    amount = amount % value.shape[0]
    return value if amount == 0 else pltpu.roll(value, amount, 0)


def offset_of(i):
    half = (i + 1) // 2
    return half * (2 * (i % 2) - 1) + NGY


def kernel(
    scalar_ref,
    vel_ref,
    out_ref,
    packed,
    send_v,
    send_n,
    send_p,
    recv_v,
    recv_n,
    recv_p,
    hal_up,
    hal_dn,
    got_up,
    got_dn,
    refine,
    coarse,
    scal,
    fine,
    field,
    edge,
    own,
    cross,
    part,
    recv_d,
    t_own,
    t_cross,
    send_o,
    send_c,
    recv_o,
    recv_c,
    joined,
    sems,
):
    gy, gz = lax.axis_index("gy"), lax.axis_index("gz")
    odd = gz % 2
    next_y, prev_y = (gy + 1) % NGY, (gy + NGY - 1) % NGY
    partner = gz + 1 - 2 * odd
    other = gz - 1 + 2 * odd
    has_other = jnp.logical_and(other >= 0, other < NGZ)
    n_other = has_other.astype(jnp.int32)
    lane = lax.broadcasted_iota(jnp.int32, (8, LANES), 1)

    barrier = pltpu.get_barrier_semaphore()

    def greet(y, z):
        pl.semaphore_signal(
            barrier, inc=1, device_id={"gy": y, "gz": z}, device_id_type=MESH
        )

    def greet_z(i, _):
        greet(gy, (gz + i) % NGZ)
        return _

    def greet_zn(i, _):
        greet(next_y, (gz + i) % NGZ)
        greet(prev_y, (gz + i) % NGZ)
        return _

    def greet_y(i, _):
        greet((gy + i) % NGY, gz)
        return _

    def greet_o(i, _):
        greet((gy + i) % NGY, other)
        return _

    lax.fori_loop(1, NGZ, greet_z, 0)
    lax.fori_loop(0, NGZ, greet_zn, 0)
    lax.fori_loop(2, NGY - 1, greet_y, 0)

    @pl.when(has_other)
    def _():
        lax.fori_loop(2, NGY - 1, greet_o, 0)

    for i in range(3):
        packed[8 + 64 * i : 72 + 64 * i, :] = vel_ref[i].T
    for z in range(NGZ):
        send_v[z, 0:4, :] = packed[8 + 4 * z : 12 + 4 * z, :]
        send_v[z, 4:8, :] = packed[72 + 4 * z : 76 + 4 * z, :]
        up = packed[135 + 4 * z : 141 + 4 * z, :] if z < NGZ - 1 else packed[135 + 4 * z : 140 + 4 * z, :]
        if z == 0:
            row = lax.broadcasted_iota(jnp.int32, up.shape, 0)
            up = jnp.where(row == 0, 0.0, up)
        if z == NGZ - 1:
            send_v[z, 8:13, :] = up
            send_v[z, 13:14, :] = jnp.zeros((1, LANES), F32)
        else:
            send_v[z, 8:14, :] = up
    lane4 = lax.broadcasted_iota(jnp.int32, (4, LANES), 1)
    for z in range(NGZ):
        first = jnp.zeros((4, LANES), F32)
        last = jnp.zeros((4, LANES), F32)
        for q in range(4):
            if q < 3:
                rows = send_v[z, 4 * q : 4 * q + 4, :]
            else:
                rows = jnp.concatenate(
                    [send_v[z, 12:14, :], jnp.zeros((2, LANES), F32)], axis=0
                )
            here = jnp.logical_and(lane4 >= 32 * q, lane4 < 32 * q + 32)
            first = jnp.where(here, lane_roll(rows, 32 * q), first)
            if q < 2:
                last = jnp.where(here, lane_roll(rows, 32 + 32 * q), last)
        send_n[z] = first
        send_p[z] = last
    for k in range(3):
        for z in range(PLANES):
            hal_up[4 * k + z : 4 * k + z + 1, :] = scalar_ref[z, k : k + 1, :]
            hal_dn[4 * k + z : 4 * k + z + 1, :] = scalar_ref[z, 21 + k : 22 + k, :]
    for z in range(PLANES):
        for t in range(TILES):
            scal[t, ROWS * z : ROWS * z + ROWS, :] = scalar_ref[
                z, :, LANES * t : LANES * t + LANES
            ]
    @pl.when(jnp.logical_not(has_other))
    def _():
        recv_c[...] = jnp.zeros_like(recv_c)

    for block in range(16):
        r = lax.broadcasted_iota(jnp.int32, (16, NX), 0) + 16 * block
        c = lax.broadcasted_iota(jnp.int32, (16, NX), 1)
        t = jnp.abs(c - 3 * r)
        if block == 0:
            t = jnp.where(r == 0, jnp.minimum(t, jnp.abs(c - NX)), t)
        refine[16 * block : 16 * block + 16, :] = (
            jnp.maximum(3 - t, 0).astype(F32).astype(BF16)
        )

    pl.semaphore_wait(barrier, 105 - 29 + 29 * n_other)

    def send_z(i, _):
        z = (gz + offset_of(i)) % NGZ
        copy_to(send_v.at[z], recv_v.at[gz], sems.at[0], sems.at[1], gy, z).start()
        return _

    def send_zn(i, _):
        z = (gz + offset_of(i)) % NGZ
        copy_to(send_n.at[z], recv_n.at[gz], sems.at[2], sems.at[3], prev_y, z).start()
        copy_to(send_p.at[z], recv_p.at[gz], sems.at[4], sems.at[5], next_y, z).start()
        return _

    lax.fori_loop(1, NGZ, send_z, 0)
    lax.fori_loop(0, NGZ, send_zn, 0)
    to_prev = copy_to(hal_up, got_dn, sems.at[6], sems.at[7], prev_y, gz)
    to_next = copy_to(hal_dn, got_up, sems.at[8], sems.at[9], next_y, gz)
    to_prev.start()
    to_next.start()
    recv_v[gz] = send_v[gz]

    wait_for(recv_v.at[0:15], sems.at[1])
    wait_for(recv_n, sems.at[3])
    wait_for(recv_p, sems.at[5])

    for c in range(8):
        for half in range(2):
            top = jnp.zeros((8, LANES), F32)
            low = jnp.zeros((6, LANES), F32)
            for i in range(8):
                g = 8 * half + i
                here = jnp.logical_and(lane >= 16 * i, lane < 16 * i + 16)
                top = jnp.where(here, lane_roll(recv_v[g, 0:8, :], 16 * (i - c)), top)
                low = jnp.where(
                    here[0:6], lane_roll(recv_v[g, 8:14, :], 16 * (i - c)), low
                )
            base = 16 * (c + 2)
            columns = pl.ds(LANES * half, LANES)
            coarse[base : base + 8, columns] = top
            coarse[base + 8 : base + 14, columns] = low
            coarse[base + 14 : base + 16, columns] = jnp.zeros((2, LANES), F32)
    for c in (-2, -1, 8, 9):
        source, offset, chunks = (recv_n, c - 8, 4) if c > 0 else (recv_p, c + 2, 2)
        base = 16 * (c + 2)
        for half in range(2):
            columns = pl.ds(LANES * half, LANES)
            for q in range(4):
                total = jnp.zeros((4, LANES), F32)
                if q < chunks:
                    for i in range(8):
                        here = jnp.logical_and(lane4 >= 16 * i, lane4 < 16 * i + 16)
                        rows = source[8 * half + i]
                        total = jnp.where(
                            here, lane_roll(rows, 16 * i - 32 * q - 16 * offset), total
                        )
                coarse[base + 4 * q : base + 4 * q + 4, columns] = total
    value = coarse[...]
    high = value.astype(BF16)
    low = (value - high.astype(F32)).astype(BF16)
    for pair in range(TILES // 2):
        weights = refine[:, 2 * LANES * pair : 2 * LANES * (pair + 1)]
        result = (
            jnp.dot(high, weights, preferred_element_type=F32)
            + jnp.dot(low, weights, preferred_element_type=F32)
        ) * (1.0 / 3.0)
        fine[2 * pair] = result[:, :LANES]
        fine[2 * pair + 1] = result[:, LANES:]

    def level(first, plane, t):
        return fine[t, pl.ds(16 * (first + 2) + plane, 8, stride=16), :]

    def edge_level(shift, plane, t):
        return jnp.concatenate(
            [
                fine[t, pl.ds(16 * (1 + shift) + plane, 4), :],
                fine[t, pl.ds(16 * (10 + shift) + plane, 4), :],
            ],
            axis=0,
        )

    def whole(load):
        return jnp.concatenate([load(t) for t in range(TILES)], axis=1)

    def spread(ref, rows, value):
        for t in range(TILES):
            ref[t, rows, :] = value[:, LANES * t : LANES * t + LANES]

    def mixed(base, following, k):
        return base if k == 0 else base * (1.0 - k / 3.0) + following * (k / 3.0)

    def sweep_x(q, u):
        d = moved_by(u, lane_roll(u, 1), lane_roll(u, -1))
        terms = products(q, d)
        total = terms[0]
        for m in (-3, -2, -1, 1, 2, 3):
            total = total + lane_roll(terms[m], m)
        return total

    for z in range(PLANES):
        base = whole(functools.partial(level, 0, z))
        following = whole(functools.partial(level, 1, z))
        for k in range(3):
            q = whole(lambda t: scal[t, pl.ds(ROWS * z + k, 8, stride=3), :])
            i = 8 * (3 * z + k)
            spread(field, slice(i, i + 8), sweep_x(q, mixed(base, following, k)))
    wait_for(got_up, sems.at[7])
    wait_for(got_dn, sems.at[9])
    base = whole(functools.partial(edge_level, 0, 0))
    following = whole(functools.partial(edge_level, 1, 0))
    for k in range(3):
        q = jnp.concatenate(
            [got_up[4 * k : 4 * k + 4, :], got_dn[4 * k : 4 * k + 4, :]], axis=0
        )
        spread(
            edge, slice(8 * k, 8 * k + 8), sweep_x(q, mixed(base, following, k))
        )

    row = lax.broadcasted_iota(jnp.int32, (8, LANES), 0)

    def phases(before, base, following, q_of):
        u = [mixed(base, following, k) for k in range(3)]
        sides = [mixed(before, base, 2)] + u + [following]
        sums = {}
        for k in range(3):
            terms = products(q_of(k), moved_by(u[k], sides[k], sides[k + 2]))
            for m in range(-3, 4):
                key = ((k + m) % 3, (k + m) // 3)
                sums[key] = terms[m] if key not in sums else sums[key] + terms[m]
        return sums

    def tile_step(t, _):
        edges = phases(
            edge_level(-1, 4, t),
            edge_level(0, 4, t),
            edge_level(1, 4, t),
            lambda k: edge[t, 8 * k : 8 * k + 8, :],
        )
        swept = {}
        for z in range(PLANES):
            sums = phases(
                level(-1, 4 + z, t),
                level(0, 4 + z, t),
                level(1, 4 + z, t),
                lambda k: field[t, 8 * (3 * z + k) : 8 * (3 * z + k) + 8, :],
            )
            for k in range(3):
                above = jnp.where(
                    row == 0, row_roll(edges[k, 1], -z), row_roll(sums[k, 1], 1)
                )
                below = jnp.where(
                    row == 7, row_roll(edges[k, -1], 3 - z), row_roll(sums[k, -1], -1)
                )
                swept[z, k] = sums[k, 0] + above + below
        lower = [level(0, 8 + p, t) for p in range(6)]
        upper = [level(1, 8 + p, t) for p in range(6)]
        for k in range(3):
            u = [mixed(lower[p], upper[p], k) for p in range(6)]
            sums = {}
            for z in range(PLANES):
                terms = products(swept[z, k], moved_by(u[z + 1], u[z], u[z + 2]))
                for m in range(-3, 4):
                    sums[z + m] = terms[m] if z + m not in sums else sums[z + m] + terms[m]
            for z in range(PLANES):
                own[t, pl.ds(ROWS * z + k, 8, stride=3), :] = sums[z]
            for i in range(3):
                up, down = sums[4 + i], sums[i - 3]
                cross[t, pl.ds(ROWS * i + k, 8, stride=3), :] = jnp.where(
                    odd == 1, up, down
                )
                part[t, pl.ds(ROWS * i + k, 8, stride=3), :] = jnp.where(
                    odd == 1, down, up
                )
        return _

    lax.fori_loop(0, TILES, tile_step, 0)

    to_partner = copy_to(part, recv_d, sems.at[10], sems.at[11], gy, partner)
    to_partner.start()

    def transposed(source, target):
        for t in range(TILES):
            target[LANES * t : LANES * t + LANES, :] = source[t].T

    def rows_of(ref, y):
        base = ROWS * y
        return [
            ref[pl.ds(pl.multiple_of(base + 8 * i, 8), 8), :] for i in range(3)
        ]

    @pl.when(has_other)
    def _():
        transposed(cross, t_cross)

        def pack(y, _):
            v = rows_of(t_cross, y)
            send_c[y, 0:8, :] = jnp.where(lane < 72, v[0], lane_roll(v[2], 72))
            send_c[y, 8:16, :] = jnp.where(lane < 72, v[1], lane_roll(v[2], 16))
            return _

        lax.fori_loop(0, NGY, pack, 0, unroll=8)

        def send(i, _):
            y = (gy + offset_of(i)) % NGY
            copy_to(
                send_c.at[y], recv_c.at[gy], sems.at[12], sems.at[13], y, other
            ).start()
            return _

        lax.fori_loop(0, NGY, send, 0)

    wait_for(recv_d, sems.at[11])
    target = pl.ds(pl.multiple_of(ROWS * (1 - odd), 8), 72)
    own[:, target, :] = own[:, target, :] + recv_d[...]
    transposed(own, t_own)

    def pack_own(y, _):
        v = rows_of(t_own, y)
        send_o[y, 0:8, :] = jnp.where(lane < 96, v[0], lane_roll(v[2], 96))
        send_o[y, 8:16, :] = jnp.where(lane < 96, v[1], lane_roll(v[2], 64))
        tail = v[2]
        tail = lane_roll(v[2], 64)
        for q in range(1, 4):
            piece = row_roll(lane_roll(v[2], 32 * q + 64), -2 * q)
            tail = jnp.where(lane < 32 * q, tail, piece)
        send_o[y, 16:18, :] = tail[0:2]
        return _

    lax.fori_loop(0, NGY, pack_own, 0, unroll=8)

    def send_own(i, _):
        y = (gy + offset_of(i)) % NGY
        copy_to(send_o.at[y], recv_o.at[gy], sems.at[14], sems.at[15], y, gz).start()
        return _

    lax.fori_loop(1, NGY, send_own, 0)
    recv_o[gy] = send_o[gy]

    @pl.when(has_other)
    def _():
        wait_for(recv_c, sems.at[13])

    wait_for(recv_o.at[0 : NGY - 1], sems.at[15])

    inside = lane - ROWS * odd
    keep = jnp.logical_and(inside >= 0, inside < 72)
    head = inside < 56

    def add_up(y, _):
        p0, p1 = recv_o[y, 0:8, :], recv_o[y, 8:16, :]
        tail = recv_o[y, 16:18, :]
        tail = jnp.concatenate([tail, tail, tail, tail], axis=0)
        last = jnp.where(lane < 32, lane_roll(p0, 32), lane_roll(p1, 64))
        end = lane_roll(tail, 64)
        for q in range(1, 4):
            end = jnp.where(row < 2 * q, end, lane_roll(tail, 64 - 32 * q))
        last = jnp.where(lane < 64, last, end)
        c0, c1 = recv_c[y, 0:8, :], recv_c[y, 8:16, :]
        turn = ROWS * odd
        e0, e1 = pltpu.roll(c0, turn, 1), pltpu.roll(c1, turn, 1)
        e2 = jnp.where(
            head, pltpu.roll(c0, turn + 56, 1), pltpu.roll(c1, (turn + 112) % LANES, 1)
        )
        joined[y, 0:8, :] = p0 + jnp.where(keep, e0, 0.0)
        joined[y, 8:16, :] = p1 + jnp.where(keep, e1, 0.0)
        joined[y, 16:24, :] = last + jnp.where(keep, e2, 0.0)
        return _

    lax.fori_loop(0, NGY, add_up, 0, unroll=8)

    def place(x, _):
        rows = pl.ds(pl.multiple_of(8 * x, 8), 8)
        for t in range(TILES):
            pieces = [None] * PLANES
            for y in range(LANES * t // ROWS, (LANES * t + LANES - 1) // ROWS + 1):
                value = joined[y, rows, :]
                edge_at = ROWS * y - LANES * t
                for z in range(PLANES):
                    turned = lane_roll(value, ROWS * (y - z))
                    pieces[z] = (
                        turned
                        if pieces[z] is None
                        else jnp.where(lane < edge_at, pieces[z], turned)
                    )
            for z in range(PLANES):
                out_ref[z, rows, LANES * t : LANES * t + LANES] = pieces[z]
        return _

    lax.fori_loop(0, 3, place, 0)

    wait_for(send_v.at[0:15], sems.at[0])
    wait_for(send_n, sems.at[2])
    wait_for(send_p, sems.at[4])
    wait_for(hal_up, sems.at[6])
    wait_for(hal_dn, sems.at[8])
    wait_for(part, sems.at[10])
    wait_for(recv_o.at[0 : NGY - 1], sems.at[14])

    @pl.when(has_other)
    def _():
        wait_for(recv_c, sems.at[12])


def local(scalar, velocity):
    vmem = pl.BlockSpec(memory_space=pltpu.VMEM)
    buffers = [
        (208, LANES),
        (NGZ, 14, LANES),
        (NGZ, 4, LANES),
        (NGZ, 4, LANES),
        (NGZ, 14, LANES),
        (NGZ, 4, LANES),
        (NGZ, 4, LANES),
        (12, NX),
        (12, NX),
        (12, NX),
        (12, NX),
    ]
    later = [
        (192, 256),
        (TILES, 96, LANES),
        (TILES, 192, LANES),
        (TILES, 96, LANES),
        (TILES, 24, LANES),
        (TILES, LANES, LANES),
        (TILES, LANES, LANES),
        (TILES, 72, LANES),
        (TILES, 72, LANES),
        (NX, LANES),
        (NX, LANES),
        (NGY, 18, LANES),
        (NGY, 16, LANES),
        (NGY, 18, LANES),
        (NGY, 16, LANES),
        (NGY, ROWS, LANES),
    ]
    return pl.pallas_call(
        kernel,
        out_shape=jax.ShapeDtypeStruct((PLANES, ROWS, NX), F32),
        in_specs=[vmem, vmem],
        out_specs=vmem,
        scratch_shapes=[pltpu.VMEM(s, F32) for s in buffers]
        + [pltpu.VMEM((256, NX), BF16)]
        + [pltpu.VMEM(s, F32) for s in later]
        + [pltpu.SemaphoreType.DMA((16,))],
        compiler_params=pltpu.CompilerParams(collective_id=0, has_side_effects=True),
    )(scalar, velocity.transpose(0, 2, 3, 1).reshape(3, LANES, 64))


def solution(mesh):
    in_specs = (P("gz", "gy", None), P(None, None, "gy", "gz"))
    out_specs = P("gz", "gy", None)
    return jax.shard_map(
        local, mesh=mesh, in_specs=in_specs, out_specs=out_specs, check_vma=False
    )
```

```python
import functools

import jax
import jax.numpy as jnp
from jax import lax
from jax.experimental import pallas as pl
from jax.experimental.pallas import tpu as pltpu
from jax.sharding import PartitionSpec as P

MESH = pl.DeviceIdType.MESH
F32 = jnp.float32
BF16 = jnp.bfloat16
NGY = 32
NGZ = 16
PLANES = 4
ROWS = 24
NX = 768
LANES = 128
TILES = NX // LANES


def copy_to(src, dst, send, recv, gy, gz):
    return pltpu.make_async_remote_copy(
        src, dst, send, recv, device_id={"gy": gy, "gz": gz}, device_id_type=MESH
    )


def wait_for(ref, sem):
    pltpu.make_async_copy(ref, ref, sem).wait()


def moved_by(speed, before, after):
    half = jnp.abs(0.5 * speed)
    return speed + half * (jnp.where(speed >= 0.0, after, before) - speed)


def products(q, d):
    a = jnp.abs(d)
    b = 1.0 - a
    w = a * b
    p3 = (w * (a * a)) * (7.0 / 24.0 - (5.0 / 24.0) * a)
    pm2 = w * (1.0 / 12.0 + a * (1.0 / 24.0 + a * (-1.0 / 3.0 + (5.0 / 24.0) * a)))
    p2 = w * (-1.0 / 12.0 + a * (-1.0 / 8.0 + a * (-3.0 / 2.0 + (25.0 / 24.0) * a)))
    pm1 = w * (-2.0 / 3.0 + (a * a) * (13.0 / 8.0 - (25.0 / 24.0) * a))
    p1 = a + pm1 + 2.0 * (pm2 - p2) - 3.0 * p3
    p0 = 1.0 - (p1 + pm1) - (p2 + pm2) - p3
    right = d >= 0.0
    q0, q1, qm1, q2, qm2, q3 = (q * p for p in (p0, p1, pm1, p2, pm2, p3))
    return {
        0: q0,
        1: jnp.where(right, q1, qm1),
        -1: jnp.where(right, qm1, q1),
        2: jnp.where(right, q2, qm2),
        -2: jnp.where(right, qm2, q2),
        3: jnp.where(right, q3, 0.0),
        -3: jnp.where(right, 0.0, q3),
    }


def lane_roll(value, amount):
    amount = amount % value.shape[-1]
    return value if amount == 0 else pltpu.roll(value, amount, value.ndim - 1)


def row_roll(value, amount):
    amount = amount % value.shape[0]
    return value if amount == 0 else pltpu.roll(value, amount, 0)


def offset_of(i):
    half = (i + 1) // 2
    return half * (2 * (i % 2) - 1) + NGY


def kernel(
    scalar_ref,
    vel_ref,
    out_ref,
    vel,
    packed,
    send_v,
    send_n,
    send_p,
    recv_v,
    recv_n,
    recv_p,
    hal_up,
    hal_dn,
    got_up,
    got_dn,
    refine,
    coarse,
    scal,
    fine,
    field,
    edge,
    own,
    cross,
    part,
    recv_d,
    t_own,
    t_cross,
    send_o,
    send_c,
    recv_o,
    recv_c,
    joined,
    sems,
):
    gy, gz = lax.axis_index("gy"), lax.axis_index("gz")
    odd = gz % 2
    next_y, prev_y = (gy + 1) % NGY, (gy + NGY - 1) % NGY
    partner = gz + 1 - 2 * odd
    other = gz - 1 + 2 * odd
    has_other = jnp.logical_and(other >= 0, other < NGZ)
    n_other = has_other.astype(jnp.int32)
    lane = lax.broadcasted_iota(jnp.int32, (8, LANES), 1)

    take_vel = pltpu.make_async_copy(vel_ref, vel, sems.at[16])
    take_vel.start()
    for t in range(TILES):
        pltpu.make_async_copy(
            scalar_ref.at[:, :, LANES * t : LANES * t + LANES], scal.at[t], sems.at[17]
        ).start()

    barrier = pltpu.get_barrier_semaphore()

    def greet(y, z):
        pl.semaphore_signal(
            barrier, inc=1, device_id={"gy": y, "gz": z}, device_id_type=MESH
        )

    def greet_z(i, _):
        greet(gy, (gz + i) % NGZ)
        return _

    def greet_zn(i, _):
        greet(next_y, (gz + i) % NGZ)
        greet(prev_y, (gz + i) % NGZ)
        return _

    def greet_y(i, _):
        greet((gy + i) % NGY, gz)
        return _

    def greet_o(i, _):
        greet((gy + i) % NGY, other)
        return _

    lax.fori_loop(0, NGZ, greet_zn, 0)
    lax.fori_loop(1, NGZ, greet_z, 0)
    lax.fori_loop(2, NGY - 1, greet_y, 0)

    @pl.when(has_other)
    def _():
        lax.fori_loop(2, NGY - 1, greet_o, 0)

    @pl.when(jnp.logical_not(has_other))
    def _():
        joined[...] = jnp.zeros_like(joined)

    for block in range(16):
        r = lax.broadcasted_iota(jnp.int32, (16, NX), 0) + 16 * block
        c = lax.broadcasted_iota(jnp.int32, (16, NX), 1)
        t = jnp.abs(c - 3 * r)
        if block == 0:
            t = jnp.where(r == 0, jnp.minimum(t, jnp.abs(c - NX)), t)
        refine[16 * block : 16 * block + 16, :] = (
            jnp.maximum(3 - t, 0).astype(F32).astype(BF16)
        )

    take_vel.wait()
    for i in range(3):
        packed[8 + 64 * i : 72 + 64 * i, :] = vel[i].T
    for z in range(NGZ):
        send_v[z, 0:4, :] = packed[8 + 4 * z : 12 + 4 * z, :]
        send_v[z, 4:8, :] = packed[72 + 4 * z : 76 + 4 * z, :]
        up = packed[135 + 4 * z : 141 + 4 * z, :] if z < NGZ - 1 else packed[135 + 4 * z : 140 + 4 * z, :]
        if z == 0:
            row = lax.broadcasted_iota(jnp.int32, up.shape, 0)
            up = jnp.where(row == 0, 0.0, up)
        if z == NGZ - 1:
            send_v[z, 8:13, :] = up
            send_v[z, 13:14, :] = jnp.zeros((1, LANES), F32)
        else:
            send_v[z, 8:14, :] = up
    lane4 = lax.broadcasted_iota(jnp.int32, (4, LANES), 1)
    for z in range(NGZ):
        first = jnp.zeros((4, LANES), F32)
        last = jnp.zeros((4, LANES), F32)
        for q in range(4):
            if q < 3:
                rows = send_v[z, 4 * q : 4 * q + 4, :]
            else:
                rows = jnp.concatenate(
                    [send_v[z, 12:14, :], jnp.zeros((2, LANES), F32)], axis=0
                )
            here = jnp.logical_and(lane4 >= 32 * q, lane4 < 32 * q + 32)
            first = jnp.where(here, lane_roll(rows, 32 * q), first)
            if q < 2:
                last = jnp.where(here, lane_roll(rows, 32 + 32 * q), last)
        send_n[z] = first
        send_p[z] = last
    wait_for(scal, sems.at[17])
    for t in range(TILES):
        columns = pl.ds(LANES * t, LANES)
        for k in range(3):
            for z in range(PLANES):
                at = slice(4 * k + z, 4 * k + z + 1)
                hal_up[at, columns] = scal[t, z, k : k + 1, :]
                hal_dn[at, columns] = scal[t, z, 21 + k : 22 + k, :]

    pl.semaphore_wait(barrier, 105 - 29 + 29 * n_other)

    def send_z(i, _):
        z = (gz + offset_of(i)) % NGZ
        copy_to(send_v.at[z], recv_v.at[gz], sems.at[0], sems.at[1], gy, z).start()
        return _

    def send_zn(i, _):
        z = (gz + offset_of(i)) % NGZ
        copy_to(send_n.at[z], recv_n.at[gz], sems.at[2], sems.at[3], prev_y, z).start()
        copy_to(send_p.at[z], recv_p.at[gz], sems.at[4], sems.at[5], next_y, z).start()
        return _

    lax.fori_loop(1, NGZ, send_z, 0)
    lax.fori_loop(0, NGZ, send_zn, 0)
    to_prev = copy_to(hal_up, got_dn, sems.at[6], sems.at[7], prev_y, gz)
    to_next = copy_to(hal_dn, got_up, sems.at[8], sems.at[9], next_y, gz)
    to_prev.start()
    to_next.start()
    recv_v[gz] = send_v[gz]

    wait_for(recv_v.at[0:15], sems.at[1])
    wait_for(recv_n, sems.at[3])
    wait_for(recv_p, sems.at[5])

    for c in range(8):
        for half in range(2):
            top = jnp.zeros((8, LANES), F32)
            low = jnp.zeros((6, LANES), F32)
            for i in range(8):
                g = 8 * half + i
                here = jnp.logical_and(lane >= 16 * i, lane < 16 * i + 16)
                top = jnp.where(here, lane_roll(recv_v[g, 0:8, :], 16 * (i - c)), top)
                low = jnp.where(
                    here[0:6], lane_roll(recv_v[g, 8:14, :], 16 * (i - c)), low
                )
            base = 16 * (c + 2)
            columns = pl.ds(LANES * half, LANES)
            coarse[base : base + 8, columns] = top
            coarse[base + 8 : base + 14, columns] = low
            coarse[base + 14 : base + 16, columns] = jnp.zeros((2, LANES), F32)
    for c in (-2, -1, 8, 9):
        source, offset, chunks = (recv_n, c - 8, 4) if c > 0 else (recv_p, c + 2, 2)
        base = 16 * (c + 2)
        for half in range(2):
            columns = pl.ds(LANES * half, LANES)
            for q in range(4):
                total = jnp.zeros((4, LANES), F32)
                if q < chunks:
                    for i in range(8):
                        here = jnp.logical_and(lane4 >= 16 * i, lane4 < 16 * i + 16)
                        rows = source[8 * half + i]
                        total = jnp.where(
                            here, lane_roll(rows, 16 * i - 32 * q - 16 * offset), total
                        )
                coarse[base + 4 * q : base + 4 * q + 4, columns] = total
    value = coarse[...]
    high = value.astype(BF16)
    low = (value - high.astype(F32)).astype(BF16)
    for pair in range(TILES // 2):
        weights = refine[:, 2 * LANES * pair : 2 * LANES * (pair + 1)]
        result = (
            jnp.dot(high, weights, preferred_element_type=F32)
            + jnp.dot(low, weights, preferred_element_type=F32)
        ) * (1.0 / 3.0)
        fine[2 * pair] = result[:, :LANES]
        fine[2 * pair + 1] = result[:, LANES:]

    def level(first, plane, t):
        return fine[t, pl.ds(16 * (first + 2) + plane, 8, stride=16), :]

    def edge_level(shift, plane, t):
        return jnp.concatenate(
            [
                fine[t, pl.ds(16 * (1 + shift) + plane, 4), :],
                fine[t, pl.ds(16 * (10 + shift) + plane, 4), :],
            ],
            axis=0,
        )

    def whole(load):
        return jnp.concatenate([load(t) for t in range(TILES)], axis=1)

    def spread(ref, rows, value):
        for t in range(TILES):
            ref[t, rows, :] = value[:, LANES * t : LANES * t + LANES]

    def mixed(base, following, k):
        return base if k == 0 else base * (1.0 - k / 3.0) + following * (k / 3.0)

    def sweep_x(q, u):
        d = moved_by(u, lane_roll(u, 1), lane_roll(u, -1))
        terms = products(q, d)
        total = terms[0]
        for m in (-3, -2, -1, 1, 2, 3):
            total = total + lane_roll(terms[m], m)
        return total

    def plane_x(z, _):
        base = whole(functools.partial(level, 0, z))
        following = whole(functools.partial(level, 1, z))
        for k in range(3):
            q = whole(lambda t: scal[t, z, pl.ds(k, 8, stride=3), :])
            rows = pl.ds(pl.multiple_of(24 * z + 8 * k, 8), 8)
            spread(field, rows, sweep_x(q, mixed(base, following, k)))
        return _

    lax.fori_loop(0, PLANES, plane_x, 0)
    wait_for(got_up, sems.at[7])
    wait_for(got_dn, sems.at[9])
    base = whole(functools.partial(edge_level, 0, 0))
    following = whole(functools.partial(edge_level, 1, 0))
    for k in range(3):
        q = jnp.concatenate(
            [got_up[4 * k : 4 * k + 4, :], got_dn[4 * k : 4 * k + 4, :]], axis=0
        )
        spread(
            edge, slice(8 * k, 8 * k + 8), sweep_x(q, mixed(base, following, k))
        )

    row = lax.broadcasted_iota(jnp.int32, (8, LANES), 0)

    def phases(before, base, following, q_of):
        u = [mixed(base, following, k) for k in range(3)]
        sides = [mixed(before, base, 2)] + u + [following]
        sums = {}
        for k in range(3):
            terms = products(q_of(k), moved_by(u[k], sides[k], sides[k + 2]))
            for m in range(-3, 4):
                key = ((k + m) % 3, (k + m) // 3)
                sums[key] = terms[m] if key not in sums else sums[key] + terms[m]
        return sums

    def tile_step(t, _):
        edges = phases(
            edge_level(-1, 4, t),
            edge_level(0, 4, t),
            edge_level(1, 4, t),
            lambda k: edge[t, 8 * k : 8 * k + 8, :],
        )
        swept = {}
        for z in range(PLANES):
            sums = phases(
                level(-1, 4 + z, t),
                level(0, 4 + z, t),
                level(1, 4 + z, t),
                lambda k: field[t, 8 * (3 * z + k) : 8 * (3 * z + k) + 8, :],
            )
            for k in range(3):
                above = jnp.where(
                    row == 0, row_roll(edges[k, 1], -z), row_roll(sums[k, 1], 1)
                )
                below = jnp.where(
                    row == 7, row_roll(edges[k, -1], 3 - z), row_roll(sums[k, -1], -1)
                )
                swept[z, k] = sums[k, 0] + above + below
        lower = [level(0, 8 + p, t) for p in range(6)]
        upper = [level(1, 8 + p, t) for p in range(6)]
        for k in range(3):
            u = [mixed(lower[p], upper[p], k) for p in range(6)]
            sums = {}
            for z in range(PLANES):
                terms = products(swept[z, k], moved_by(u[z + 1], u[z], u[z + 2]))
                for m in range(-3, 4):
                    sums[z + m] = terms[m] if z + m not in sums else sums[z + m] + terms[m]
            for z in range(PLANES):
                own[t, pl.ds(ROWS * z + k, 8, stride=3), :] = sums[z]
            for i in range(3):
                up, down = sums[4 + i], sums[i - 3]
                cross[t, pl.ds(ROWS * i + k, 8, stride=3), :] = jnp.where(
                    odd == 1, up, down
                )
                part[t, pl.ds(ROWS * i + k, 8, stride=3), :] = jnp.where(
                    odd == 1, down, up
                )
        return _

    def transposed(source, target, h):
        for i in range(TILES // 2):
            t = TILES // 2 * h + i
            rows = pl.ds(pl.multiple_of(LANES * t, LANES), LANES)
            target[rows, :] = source[t].T

    def rows_of(ref, y):
        base = ROWS * y
        return [
            ref[pl.ds(pl.multiple_of(base + 8 * i, 8), 8), :] for i in range(3)
        ]

    def in_groups(pack, send, h):
        def order(i):
            return NGY // 2 * h + (gy + offset_of((i + 1) % 16)) % (NGY // 2)

        for n in range(2):
            for i in range(8):
                pack(order(8 * n + i))
            if n:
                for i in range(8):
                    send(order(i))
        for i in range(8):
            send(order(i + 8))

    def pack_cross(y):
        v = rows_of(t_cross, y)
        send_c[y, 0:8, :] = jnp.where(lane < 72, v[0], lane_roll(v[2], 72))
        low = jnp.where(lane < 72, v[1], lane_roll(v[2], 16))
        low = jnp.where(lane < 88, low, row_roll(lane_roll(v[2], 32), -6))
        for q in range(3):
            piece = row_roll(lane_roll(v[1], 104 - 24 * q), 2 * q - 6)
            here = lane >= 104 if q == 0 else jnp.logical_and(lane >= 104, row >= 2 * q)
            low = jnp.where(here, piece, low)
        send_c[y, 8:14, :] = low[0:6]

    def send_cross(y):
        copy_to(
            send_c.at[y], recv_c.at[gy], sems.at[12], sems.at[13], y, other
        ).start()

    def pack_own(y):
        v = rows_of(t_own, y)
        send_o[y, 0:8, :] = jnp.where(lane < 96, v[0], lane_roll(v[2], 96))
        send_o[y, 8:16, :] = jnp.where(lane < 96, v[1], lane_roll(v[2], 64))
        tail = lane_roll(v[2], 64)
        for q in range(1, 4):
            piece = row_roll(lane_roll(v[2], 32 * q + 64), -2 * q)
            tail = jnp.where(lane < 32 * q, tail, piece)
        send_o[y, 16:18, :] = tail[0:2]

    def send_own(y):
        @pl.when(y != gy)
        def _():
            copy_to(
                send_o.at[y], recv_o.at[gy], sems.at[14], sems.at[15], y, gz
            ).start()

    def half_of(ref, h):
        return ref.at[pl.ds(TILES // 2 * h, TILES // 2)]

    def cross_step(step, carry):
        h = (gy + step) % 2

        def tiles(i, _):
            return tile_step(TILES // 2 * h + i, _)

        lax.fori_loop(0, TILES // 2, tiles, 0)
        copy_to(
            half_of(part, h), half_of(recv_d, h), sems.at[10], sems.at[18 + step], gy, partner
        ).start()

        @pl.when(has_other)
        def _():
            transposed(cross, t_cross, h)
            in_groups(pack_cross, send_cross, h)

        return carry

    lax.fori_loop(0, 2, cross_step, 0)

    target = pl.ds(pl.multiple_of(ROWS * (1 - odd), 8), 72)

    def own_step(step, _):
        h = (gy + step) % 2
        wait_for(half_of(recv_d, h), sems.at[18 + step])
        tiles = pl.ds(TILES // 2 * h, TILES // 2)
        own[tiles, target, :] = own[tiles, target, :] + recv_d[tiles]
        transposed(own, t_own, h)
        in_groups(pack_own, send_own, h)
        return _

    lax.fori_loop(0, 2, own_step, 0)
    recv_o[gy] = send_o[gy]

    inside = lane - ROWS * odd
    keep = jnp.logical_and(inside >= 0, inside < 72)
    head = inside < 56

    @pl.when(has_other)
    def _():
        wait_for(recv_c, sems.at[13])

        turn = ROWS * odd

        def turned(value, amount):
            return pltpu.roll(value, (turn + amount) % LANES, 1)

        def open_cross(y, _):
            c0 = recv_c[y, 0:8, :]
            c1 = jnp.concatenate(
                [recv_c[y, 8:14, :], jnp.zeros((2, LANES), F32)], axis=0
            )
            tail = turned(row_roll(c1, 6), 24)
            for q in range(1, 3):
                piece = turned(row_roll(c1, 6 - 2 * q), 24 * q + 24)
                tail = jnp.where(inside < 24 * q, tail, piece)
            end = jnp.where(row < 6, turned(c1, 112), turned(row_roll(c1, 6), 96))
            e1 = jnp.where(row < 6, turned(c1, 0), tail)
            e2 = jnp.where(head, turned(c0, 56), end)
            joined[y, 0:8, :] = jnp.where(keep, turned(c0, 0), 0.0)
            joined[y, 8:16, :] = jnp.where(keep, e1, 0.0)
            joined[y, 16:24, :] = jnp.where(keep, e2, 0.0)
            return _

        lax.fori_loop(0, NGY, open_cross, 0, unroll=8)

    wait_for(recv_o.at[0 : NGY - 1], sems.at[15])

    def add_up(y, _):
        p0, p1 = recv_o[y, 0:8, :], recv_o[y, 8:16, :]
        tail = recv_o[y, 16:18, :]
        tail = jnp.concatenate([tail, tail, tail, tail], axis=0)
        last = jnp.where(lane < 32, lane_roll(p0, 32), lane_roll(p1, 64))
        end = lane_roll(tail, 64)
        for q in range(1, 4):
            end = jnp.where(row < 2 * q, end, lane_roll(tail, 64 - 32 * q))
        last = jnp.where(lane < 64, last, end)
        joined[y, 0:8, :] = joined[y, 0:8, :] + p0
        joined[y, 8:16, :] = joined[y, 8:16, :] + p1
        joined[y, 16:24, :] = joined[y, 16:24, :] + last
        return _

    lax.fori_loop(0, NGY, add_up, 0, unroll=8)

    def place(x, _):
        rows = pl.ds(pl.multiple_of(8 * x, 8), 8)
        for t in range(TILES):
            pieces = [None] * PLANES
            for y in range(LANES * t // ROWS, (LANES * t + LANES - 1) // ROWS + 1):
                value = joined[y, rows, :]
                edge_at = ROWS * y - LANES * t
                for z in range(PLANES):
                    turned = lane_roll(value, ROWS * (y - z))
                    pieces[z] = (
                        turned
                        if pieces[z] is None
                        else jnp.where(lane < edge_at, pieces[z], turned)
                    )
            for z in range(PLANES):
                out_ref[z, rows, LANES * t : LANES * t + LANES] = pieces[z]
        return _

    lax.fori_loop(0, 3, place, 0)

    wait_for(send_v.at[0:15], sems.at[0])
    wait_for(send_n, sems.at[2])
    wait_for(send_p, sems.at[4])
    wait_for(hal_up, sems.at[6])
    wait_for(hal_dn, sems.at[8])
    wait_for(part, sems.at[10])
    wait_for(recv_o.at[0 : NGY - 1], sems.at[14])

    @pl.when(has_other)
    def _():
        wait_for(recv_c, sems.at[12])


def local(scalar, velocity):
    vmem = pl.BlockSpec(memory_space=pltpu.VMEM)
    buffers = [
        (3, LANES, 64),
        (208, LANES),
        (NGZ, 14, LANES),
        (NGZ, 4, LANES),
        (NGZ, 4, LANES),
        (NGZ, 14, LANES),
        (NGZ, 4, LANES),
        (NGZ, 4, LANES),
        (12, NX),
        (12, NX),
        (12, NX),
        (12, NX),
    ]
    later = [
        (192, 256),
        (TILES, PLANES, ROWS, LANES),
        (TILES, 192, LANES),
        (TILES, 96, LANES),
        (TILES, 24, LANES),
        (TILES, LANES, LANES),
        (TILES, LANES, LANES),
        (TILES, 72, LANES),
        (TILES, 72, LANES),
        (NX, LANES),
        (NX, LANES),
        (NGY, 18, LANES),
        (NGY, 14, LANES),
        (NGY, 18, LANES),
        (NGY, 14, LANES),
        (NGY, ROWS, LANES),
    ]
    return pl.pallas_call(
        kernel,
        out_shape=pltpu.VMEM((PLANES, ROWS, NX), F32),
        in_specs=[pl.BlockSpec(memory_space=pl.ANY)] * 2,
        out_specs=vmem,
        scratch_shapes=[pltpu.VMEM(s, F32) for s in buffers]
        + [pltpu.VMEM((256, NX), BF16)]
        + [pltpu.VMEM(s, F32) for s in later]
        + [pltpu.SemaphoreType.DMA((20,))],
        compiler_params=pltpu.CompilerParams(collective_id=0, has_side_effects=True),
    )(scalar, velocity.transpose(0, 2, 3, 1).reshape(3, LANES, 64))


def solution(mesh):
    in_specs = (P("gz", "gy", None), P(None, None, "gy", "gz"))
    out_specs = P("gz", "gy", None)
    return jax.shard_map(
        local, mesh=mesh, in_specs=in_specs, out_specs=out_specs, check_vma=False
    )
```

```python
import functools

import jax
import jax.numpy as jnp
from jax import lax
from jax.experimental import pallas as pl
from jax.experimental.pallas import tpu as pltpu
from jax.sharding import PartitionSpec as P

MESH = pl.DeviceIdType.MESH
F32 = jnp.float32
BF16 = jnp.bfloat16
NGY = 32
NGZ = 16
PLANES = 4
ROWS = 24
NX = 768
LANES = 128
TILES = NX // LANES


def copy_to(src, dst, send, recv, gy, gz):
    return pltpu.make_async_remote_copy(
        src, dst, send, recv, device_id={"gy": gy, "gz": gz}, device_id_type=MESH
    )


def wait_for(ref, sem):
    pltpu.make_async_copy(ref, ref, sem).wait()


def moved_by(speed, before, after):
    half = jnp.abs(0.5 * speed)
    return speed + half * (jnp.where(speed >= 0.0, after, before) - speed)


def products(q, d):
    a = jnp.abs(d)
    d2 = d * d
    d3 = d2 * d
    s = (d3 - d) * (1.0 / 12.0)
    half = 0.5 * d
    r = s * half
    odd3 = d3 * ((1.0 - a) * (7.0 / 48.0 - (5.0 / 48.0) * a))
    even3 = jnp.abs(odd3)
    even2 = r - 6.0 * even3
    odd2 = s - 4.0 * odd3
    even1 = (0.5 * d2 - 4.0 * r) + 15.0 * even3
    odd1 = (half - 2.0 * s) + 5.0 * odd3
    middle = 1.0 - 2.0 * ((even1 + even2) + even3)
    return {
        0: q * middle,
        1: q * (even1 + odd1),
        -1: q * (even1 - odd1),
        2: q * (even2 + odd2),
        -2: q * (even2 - odd2),
        3: q * (even3 + odd3),
        -3: q * (even3 - odd3),
    }


def lane_roll(value, amount):
    amount = amount % value.shape[-1]
    return value if amount == 0 else pltpu.roll(value, amount, value.ndim - 1)


def row_roll(value, amount):
    amount = amount % value.shape[0]
    return value if amount == 0 else pltpu.roll(value, amount, 0)


def offset_of(i):
    half = (i + 1) // 2
    return half * (2 * (i % 2) - 1) + NGY


def kernel(
    scalar_ref,
    vel_ref,
    out_ref,
    vel,
    packed,
    send_v,
    send_n,
    send_p,
    recv_v,
    recv_n,
    recv_p,
    hal_up,
    hal_dn,
    got_up,
    got_dn,
    refine,
    coarse,
    scal,
    fine,
    field,
    edge,
    own,
    cross,
    part,
    recv_d,
    t_own,
    t_cross,
    send_o,
    send_c,
    recv_o,
    recv_c,
    joined,
    sems,
    column,
):
    gy, gz = lax.axis_index("gy"), lax.axis_index("gz")
    odd = gz % 2
    next_y, prev_y = (gy + 1) % NGY, (gy + NGY - 1) % NGY
    partner = gz + 1 - 2 * odd
    other = gz - 1 + 2 * odd
    has_other = jnp.logical_and(other >= 0, other < NGZ)
    lane = lax.broadcasted_iota(jnp.int32, (8, LANES), 1)

    take_vel = pltpu.make_async_copy(vel_ref, vel, sems.at[16])
    take_vel.start()
    for t in range(TILES):
        pltpu.make_async_copy(
            scalar_ref.at[:, :, LANES * t : LANES * t + LANES], scal.at[t], sems.at[17]
        ).start()

    barrier = pltpu.get_barrier_semaphore()

    def greet(y, z):
        pl.semaphore_signal(
            barrier, inc=1, device_id={"gy": y, "gz": z}, device_id_type=MESH
        )

    def greet_z(i, _):
        greet(gy, (gz + i) % NGZ)
        return _

    def greet_zn(i, _):
        greet(next_y, (gz + i) % NGZ)
        greet(prev_y, (gz + i) % NGZ)
        return _

    def greet_y(i, _):
        greet((gy + i) % NGY, gz)
        return _

    lax.fori_loop(0, NGZ, greet_zn, 0)
    lax.fori_loop(1, NGZ, greet_z, 0)
    lax.fori_loop(2, NGY - 1, greet_y, 0)

    @pl.when(jnp.logical_not(has_other))
    def _():
        joined[...] = jnp.zeros_like(joined)

    for block in range(16):
        r = lax.broadcasted_iota(jnp.int32, (16, NX), 0) + 16 * block
        c = lax.broadcasted_iota(jnp.int32, (16, NX), 1)
        t = jnp.abs(c - 3 * r)
        if block == 0:
            t = jnp.where(r == 0, jnp.minimum(t, jnp.abs(c - NX)), t)
        refine[16 * block : 16 * block + 16, :] = (
            jnp.maximum(3 - t, 0).astype(F32).astype(BF16)
        )

    take_vel.wait()
    for i in range(3):
        packed[8 + 64 * i : 72 + 64 * i, :] = vel[i].T
    for z in range(NGZ):
        send_v[z, 0:4, :] = packed[8 + 4 * z : 12 + 4 * z, :]
        send_v[z, 4:8, :] = packed[72 + 4 * z : 76 + 4 * z, :]
        up = packed[135 + 4 * z : 141 + 4 * z, :] if z < NGZ - 1 else packed[135 + 4 * z : 140 + 4 * z, :]
        if z == 0:
            row = lax.broadcasted_iota(jnp.int32, up.shape, 0)
            up = jnp.where(row == 0, 0.0, up)
        if z == NGZ - 1:
            send_v[z, 8:13, :] = up
            send_v[z, 13:14, :] = jnp.zeros((1, LANES), F32)
        else:
            send_v[z, 8:14, :] = up
    lane4 = lax.broadcasted_iota(jnp.int32, (4, LANES), 1)
    for z in range(NGZ):
        first = jnp.zeros((4, LANES), F32)
        last = jnp.zeros((4, LANES), F32)
        for q in range(4):
            if q < 3:
                rows = send_v[z, 4 * q : 4 * q + 4, :]
            else:
                rows = jnp.concatenate(
                    [send_v[z, 12:14, :], jnp.zeros((2, LANES), F32)], axis=0
                )
            here = jnp.logical_and(lane4 >= 32 * q, lane4 < 32 * q + 32)
            first = jnp.where(here, lane_roll(rows, 32 * q), first)
            if q < 2:
                last = jnp.where(here, lane_roll(rows, 32 + 32 * q), last)
        send_n[z] = first
        send_p[z] = last
    wait_for(scal, sems.at[17])
    for t in range(TILES):
        columns = pl.ds(LANES * t, LANES)
        for k in range(3):
            for z in range(PLANES):
                at = slice(4 * k + z, 4 * k + z + 1)
                hal_up[at, columns] = scal[t, z, k : k + 1, :]
                hal_dn[at, columns] = scal[t, z, 21 + k : 22 + k, :]

    pl.semaphore_wait(barrier, 76)

    @pl.when(has_other)
    def _():
        pl.semaphore_signal(
            column, inc=1, device_id={"gy": gy, "gz": other}, device_id_type=MESH
        )


    def send_z(i, _):
        z = (gz + offset_of(i)) % NGZ
        copy_to(send_v.at[z], recv_v.at[gz], sems.at[0], sems.at[1], gy, z).start()
        return _

    def send_zn(i, _):
        z = (gz + offset_of(i)) % NGZ
        copy_to(send_n.at[z], recv_n.at[gz], sems.at[2], sems.at[3], prev_y, z).start()
        copy_to(send_p.at[z], recv_p.at[gz], sems.at[4], sems.at[5], next_y, z).start()
        return _

    lax.fori_loop(1, NGZ, send_z, 0)
    lax.fori_loop(0, NGZ, send_zn, 0)
    to_prev = copy_to(hal_up, got_dn, sems.at[6], sems.at[7], prev_y, gz)
    to_next = copy_to(hal_dn, got_up, sems.at[8], sems.at[9], next_y, gz)
    to_prev.start()
    to_next.start()
    recv_v[gz] = send_v[gz]

    wait_for(recv_v.at[0:15], sems.at[1])
    wait_for(recv_n, sems.at[3])
    wait_for(recv_p, sems.at[5])

    for c in range(8):
        for half in range(2):
            top = jnp.zeros((8, LANES), F32)
            low = jnp.zeros((6, LANES), F32)
            for i in range(8):
                g = 8 * half + i
                here = jnp.logical_and(lane >= 16 * i, lane < 16 * i + 16)
                top = jnp.where(here, lane_roll(recv_v[g, 0:8, :], 16 * (i - c)), top)
                low = jnp.where(
                    here[0:6], lane_roll(recv_v[g, 8:14, :], 16 * (i - c)), low
                )
            base = 16 * (c + 2)
            columns = pl.ds(LANES * half, LANES)
            coarse[base : base + 8, columns] = top
            coarse[base + 8 : base + 14, columns] = low
            coarse[base + 14 : base + 16, columns] = jnp.zeros((2, LANES), F32)
    for c in (-2, -1, 8, 9):
        source, offset, chunks = (recv_n, c - 8, 4) if c > 0 else (recv_p, c + 2, 2)
        base = 16 * (c + 2)
        for half in range(2):
            columns = pl.ds(LANES * half, LANES)
            for q in range(4):
                total = jnp.zeros((4, LANES), F32)
                if q < chunks:
                    for i in range(8):
                        here = jnp.logical_and(lane4 >= 16 * i, lane4 < 16 * i + 16)
                        rows = source[8 * half + i]
                        total = jnp.where(
                            here, lane_roll(rows, 16 * i - 32 * q - 16 * offset), total
                        )
                coarse[base + 4 * q : base + 4 * q + 4, columns] = total
    value = coarse[...]
    high = value.astype(BF16)
    low = (value - high.astype(F32)).astype(BF16)
    for pair in range(TILES // 2):
        weights = refine[:, 2 * LANES * pair : 2 * LANES * (pair + 1)]
        result = (
            jnp.dot(high, weights, preferred_element_type=F32)
            + jnp.dot(low, weights, preferred_element_type=F32)
        ) * (1.0 / 3.0)
        fine[2 * pair] = result[:, :LANES]
        fine[2 * pair + 1] = result[:, LANES:]

    def level(first, plane, t):
        return fine[t, pl.ds(16 * (first + 2) + plane, 8, stride=16), :]

    def edge_level(shift, plane, t):
        return jnp.concatenate(
            [
                fine[t, pl.ds(16 * (1 + shift) + plane, 4), :],
                fine[t, pl.ds(16 * (10 + shift) + plane, 4), :],
            ],
            axis=0,
        )

    def whole(load):
        return jnp.concatenate([load(t) for t in range(TILES)], axis=1)

    def spread(ref, rows, value):
        for t in range(TILES):
            ref[t, rows, :] = value[:, LANES * t : LANES * t + LANES]

    def mixed(base, following, k):
        return base if k == 0 else base * (1.0 - k / 3.0) + following * (k / 3.0)

    def sweep_x(q, u):
        d = moved_by(u, lane_roll(u, 1), lane_roll(u, -1))
        terms = products(q, d)
        total = terms[0]
        for m in (-3, -2, -1, 1, 2, 3):
            total = total + lane_roll(terms[m], m)
        return total

    def plane_x(z, _):
        base = whole(functools.partial(level, 0, z))
        following = whole(functools.partial(level, 1, z))
        for k in range(3):
            q = whole(lambda t: scal[t, z, pl.ds(k, 8, stride=3), :])
            rows = pl.ds(pl.multiple_of(24 * z + 8 * k, 8), 8)
            spread(field, rows, sweep_x(q, mixed(base, following, k)))
        return _

    lax.fori_loop(0, PLANES, plane_x, 0)
    wait_for(got_up, sems.at[7])
    wait_for(got_dn, sems.at[9])
    base = whole(functools.partial(edge_level, 0, 0))
    following = whole(functools.partial(edge_level, 1, 0))
    for k in range(3):
        q = jnp.concatenate(
            [got_up[4 * k : 4 * k + 4, :], got_dn[4 * k : 4 * k + 4, :]], axis=0
        )
        spread(
            edge, slice(8 * k, 8 * k + 8), sweep_x(q, mixed(base, following, k))
        )

    row = lax.broadcasted_iota(jnp.int32, (8, LANES), 0)

    def phases(before, base, following, q_of):
        u = [mixed(base, following, k) for k in range(3)]
        sides = [mixed(before, base, 2)] + u + [following]
        sums = {}
        for k in range(3):
            terms = products(q_of(k), moved_by(u[k], sides[k], sides[k + 2]))
            for m in range(-3, 4):
                key = ((k + m) % 3, (k + m) // 3)
                sums[key] = terms[m] if key not in sums else sums[key] + terms[m]
        return sums

    def tile_step(t, _):
        edges = phases(
            edge_level(-1, 4, t),
            edge_level(0, 4, t),
            edge_level(1, 4, t),
            lambda k: edge[t, 8 * k : 8 * k + 8, :],
        )
        swept = {}
        for z in range(PLANES):
            sums = phases(
                level(-1, 4 + z, t),
                level(0, 4 + z, t),
                level(1, 4 + z, t),
                lambda k: field[t, 8 * (3 * z + k) : 8 * (3 * z + k) + 8, :],
            )
            for k in range(3):
                above = jnp.where(
                    row == 0, row_roll(edges[k, 1], -z), row_roll(sums[k, 1], 1)
                )
                below = jnp.where(
                    row == 7, row_roll(edges[k, -1], 3 - z), row_roll(sums[k, -1], -1)
                )
                swept[z, k] = sums[k, 0] + above + below
        lower = [level(0, 8 + p, t) for p in range(6)]
        upper = [level(1, 8 + p, t) for p in range(6)]
        for k in range(3):
            u = [mixed(lower[p], upper[p], k) for p in range(6)]
            sums = {}
            for z in range(PLANES):
                terms = products(swept[z, k], moved_by(u[z + 1], u[z], u[z + 2]))
                for m in range(-3, 4):
                    sums[z + m] = terms[m] if z + m not in sums else sums[z + m] + terms[m]
            for z in range(PLANES):
                own[t, pl.ds(ROWS * z + k, 8, stride=3), :] = sums[z]
            for i in range(3):
                up, down = sums[4 + i], sums[i - 3]
                cross[t, pl.ds(ROWS * i + k, 8, stride=3), :] = jnp.where(
                    odd == 1, up, down
                )
                part[t, pl.ds(ROWS * i + k, 8, stride=3), :] = jnp.where(
                    odd == 1, down, up
                )
        return _

    def transposed(source, target, h):
        for i in range(TILES // 2):
            t = TILES // 2 * h + i
            rows = pl.ds(pl.multiple_of(LANES * t, LANES), LANES)
            target[rows, :] = source[t].T

    def rows_of(ref, y):
        base = ROWS * y
        return [
            ref[pl.ds(pl.multiple_of(base + 8 * i, 8), 8), :] for i in range(3)
        ]

    def in_groups(pack, send, h):
        def order(i):
            return NGY // 2 * h + (gy + offset_of((i + 1) % 16)) % (NGY // 2)

        for n in range(2):
            for i in range(8):
                pack(order(8 * n + i))
            if n:
                for i in range(8):
                    send(order(i))
        for i in range(8):
            send(order(i + 8))

    def pack_cross(y):
        v = rows_of(t_cross, y)
        send_c[y, 0:8, :] = jnp.where(lane < 72, v[0], lane_roll(v[2], 72))
        low = jnp.where(lane < 72, v[1], lane_roll(v[2], 16))
        low = jnp.where(lane < 88, low, row_roll(lane_roll(v[2], 32), -6))
        for q in range(3):
            piece = row_roll(lane_roll(v[1], 104 - 24 * q), 2 * q - 6)
            here = lane >= 104 if q == 0 else jnp.logical_and(lane >= 104, row >= 2 * q)
            low = jnp.where(here, piece, low)
        send_c[y, 8:14, :] = low[0:6]

    def send_cross(y):
        copy_to(
            send_c.at[y], recv_c.at[gy], sems.at[12], sems.at[13], y, other
        ).start()

    def pack_own(y):
        v = rows_of(t_own, y)
        send_o[y, 0:8, :] = jnp.where(lane < 96, v[0], lane_roll(v[2], 96))
        send_o[y, 8:16, :] = jnp.where(lane < 96, v[1], lane_roll(v[2], 64))
        tail = lane_roll(v[2], 64)
        for q in range(1, 4):
            piece = row_roll(lane_roll(v[2], 32 * q + 64), -2 * q)
            tail = jnp.where(lane < 32 * q, tail, piece)
        send_o[y, 16:18, :] = tail[0:2]

    def send_own(y):
        @pl.when(y != gy)
        def _():
            copy_to(
                send_o.at[y], recv_o.at[gy], sems.at[14], sems.at[15], y, gz
            ).start()

    def half_of(ref, h):
        return ref.at[pl.ds(TILES // 2 * h, TILES // 2)]

    def cross_step(step, carry):
        h = (gy + step) % 2

        def tiles(i, _):
            return tile_step(TILES // 2 * h + i, _)

        lax.fori_loop(0, TILES // 2, tiles, 0)
        copy_to(
            half_of(part, h), half_of(recv_d, h), sems.at[10], sems.at[18 + step], gy, partner
        ).start()

        @pl.when(has_other)
        def _():
            transposed(cross, t_cross, h)
            in_groups(pack_cross, send_cross, h)

        return carry

    @pl.when(has_other)
    def _():
        pl.semaphore_wait(column, 1)

    lax.fori_loop(0, 2, cross_step, 0)

    target = pl.ds(pl.multiple_of(ROWS * (1 - odd), 8), 72)

    def own_step(step, _):
        h = (gy + step) % 2
        wait_for(half_of(recv_d, h), sems.at[18 + step])
        tiles = pl.ds(TILES // 2 * h, TILES // 2)
        own[tiles, target, :] = own[tiles, target, :] + recv_d[tiles]
        transposed(own, t_own, h)
        in_groups(pack_own, send_own, h)
        return _

    lax.fori_loop(0, 2, own_step, 0)
    recv_o[gy] = send_o[gy]

    inside = lane - ROWS * odd
    keep = jnp.logical_and(inside >= 0, inside < 72)
    head = inside < 56

    @pl.when(has_other)
    def _():
        wait_for(recv_c, sems.at[13])

        turn = ROWS * odd

        def turned(value, amount):
            return pltpu.roll(value, (turn + amount) % LANES, 1)

        def open_cross(y, _):
            c0 = recv_c[y, 0:8, :]
            c1 = jnp.concatenate(
                [recv_c[y, 8:14, :], jnp.zeros((2, LANES), F32)], axis=0
            )
            tail = turned(row_roll(c1, 6), 24)
            for q in range(1, 3):
                piece = turned(row_roll(c1, 6 - 2 * q), 24 * q + 24)
                tail = jnp.where(inside < 24 * q, tail, piece)
            end = jnp.where(row < 6, turned(c1, 112), turned(row_roll(c1, 6), 96))
            e1 = jnp.where(row < 6, turned(c1, 0), tail)
            e2 = jnp.where(head, turned(c0, 56), end)
            joined[y, 0:8, :] = jnp.where(keep, turned(c0, 0), 0.0)
            joined[y, 8:16, :] = jnp.where(keep, e1, 0.0)
            joined[y, 16:24, :] = jnp.where(keep, e2, 0.0)
            return _

        lax.fori_loop(0, NGY, open_cross, 0, unroll=8)

    wait_for(recv_o.at[0 : NGY - 1], sems.at[15])

    def last_rows(y):
        p0, p1 = recv_o[y, 0:8, :], recv_o[y, 8:16, :]
        tail = recv_o[y, 16:18, :]
        tail = jnp.concatenate([tail, tail, tail, tail], axis=0)
        last = jnp.where(lane < 32, lane_roll(p0, 32), lane_roll(p1, 64))
        end = lane_roll(tail, 64)
        for q in range(1, 4):
            end = jnp.where(row < 2 * q, end, lane_roll(tail, 64 - 32 * q))
        return jnp.where(lane < 64, last, end)

    for y in range(NGY):
        joined[y, 16:24, :] = joined[y, 16:24, :] + last_rows(y)
    for x in range(3):
        rows = slice(8 * x, 8 * x + 8)
        for t in range(TILES):
            pieces = [None] * PLANES
            for y in range(LANES * t // ROWS, (LANES * t + LANES - 1) // ROWS + 1):
                value = joined[y, rows, :]
                if x < 2:
                    value = value + recv_o[y, rows, :]
                edge_at = ROWS * y - LANES * t
                for z in range(PLANES):
                    turned_to = lane_roll(value, ROWS * (y - z))
                    pieces[z] = (
                        turned_to
                        if pieces[z] is None
                        else jnp.where(lane < edge_at, pieces[z], turned_to)
                    )
            for z in range(PLANES):
                out_ref[z, rows, LANES * t : LANES * t + LANES] = pieces[z]

    wait_for(send_v.at[0:15], sems.at[0])
    wait_for(send_n, sems.at[2])
    wait_for(send_p, sems.at[4])
    wait_for(hal_up, sems.at[6])
    wait_for(hal_dn, sems.at[8])
    wait_for(part, sems.at[10])
    wait_for(recv_o.at[0 : NGY - 1], sems.at[14])

    @pl.when(has_other)
    def _():
        wait_for(recv_c, sems.at[12])


def local(scalar, velocity):
    vmem = pl.BlockSpec(memory_space=pltpu.VMEM)
    buffers = [
        (3, LANES, 64),
        (208, LANES),
        (NGZ, 14, LANES),
        (NGZ, 4, LANES),
        (NGZ, 4, LANES),
        (NGZ, 14, LANES),
        (NGZ, 4, LANES),
        (NGZ, 4, LANES),
        (12, NX),
        (12, NX),
        (12, NX),
        (12, NX),
    ]
    later = [
        (192, 256),
        (TILES, PLANES, ROWS, LANES),
        (TILES, 192, LANES),
        (TILES, 96, LANES),
        (TILES, 24, LANES),
        (TILES, LANES, LANES),
        (TILES, LANES, LANES),
        (TILES, 72, LANES),
        (TILES, 72, LANES),
        (NX, LANES),
        (NX, LANES),
        (NGY, 18, LANES),
        (NGY, 14, LANES),
        (NGY, 18, LANES),
        (NGY, 14, LANES),
        (NGY, ROWS, LANES),
    ]
    return pl.pallas_call(
        kernel,
        out_shape=pltpu.VMEM((PLANES, ROWS, NX), F32),
        in_specs=[pl.BlockSpec(memory_space=pl.ANY)] * 2,
        out_specs=vmem,
        scratch_shapes=[pltpu.VMEM(s, F32) for s in buffers]
        + [pltpu.VMEM((256, NX), BF16)]
        + [pltpu.VMEM(s, F32) for s in later]
        + [pltpu.SemaphoreType.DMA((20,)), pltpu.SemaphoreType.REGULAR],
        compiler_params=pltpu.CompilerParams(collective_id=0, has_side_effects=True),
    )(scalar, velocity.transpose(0, 2, 3, 1).reshape(3, LANES, 64))


def solution(mesh):
    in_specs = (P("gz", "gy", None), P(None, None, "gy", "gz"))
    out_specs = P("gz", "gy", None)
    return jax.shard_map(
        local, mesh=mesh, in_specs=in_specs, out_specs=out_specs, check_vma=False
    )
```

```python
import functools

import jax
import jax.numpy as jnp
from jax import lax
from jax.experimental import pallas as pl
from jax.experimental.pallas import tpu as pltpu
from jax.sharding import PartitionSpec as P

MESH = pl.DeviceIdType.MESH
F32 = jnp.float32
BF16 = jnp.bfloat16
NGY = 32
NGZ = 16
PLANES = 4
ROWS = 24
NX = 768
LANES = 128
TILES = NX // LANES


def copy_to(src, dst, send, recv, gy, gz):
    return pltpu.make_async_remote_copy(
        src, dst, send, recv, device_id={"gy": gy, "gz": gz}, device_id_type=MESH
    )


def wait_for(ref, sem):
    pltpu.make_async_copy(ref, ref, sem).wait()


def moved_by(speed, before, after):
    half = jnp.abs(0.5 * speed)
    return speed + half * (jnp.where(speed >= 0.0, after, before) - speed)


def products(q, d):
    a = jnp.abs(d)
    d2 = d * d
    d3 = d2 * d
    s = (d3 - d) * (1.0 / 12.0)
    half = 0.5 * d
    r = s * half
    odd3 = d3 * ((1.0 - a) * (7.0 / 48.0 - (5.0 / 48.0) * a))
    even3 = jnp.abs(odd3)
    even2 = r - 6.0 * even3
    odd2 = s - 4.0 * odd3
    even1 = (0.5 * d2 - 4.0 * r) + 15.0 * even3
    odd1 = (half - 2.0 * s) + 5.0 * odd3
    middle = 1.0 - 2.0 * ((even1 + even2) + even3)
    return {
        0: q * middle,
        1: q * (even1 + odd1),
        -1: q * (even1 - odd1),
        2: q * (even2 + odd2),
        -2: q * (even2 - odd2),
        3: q * (even3 + odd3),
        -3: q * (even3 - odd3),
    }


def lane_roll(value, amount):
    amount = amount % value.shape[-1]
    return value if amount == 0 else pltpu.roll(value, amount, value.ndim - 1)


def row_roll(value, amount):
    amount = amount % value.shape[0]
    return value if amount == 0 else pltpu.roll(value, amount, 0)


def exchanged(values, width, lane):
    values = list(values)
    step = len(values) // 2
    while step:
        stay = jnp.zeros(lane.shape, jnp.bool_)
        for c in range(len(values)):
            if not c & step:
                stay = jnp.logical_or(
                    stay, jnp.logical_and(lane >= width * c, lane < width * (c + 1))
                )
        for i in range(len(values)):
            if not i & step:
                a, b = values[i], values[i + step]
                values[i] = jnp.where(stay, a, lane_roll(b, width * step))
                values[i + step] = jnp.where(stay, lane_roll(a, -width * step), b)
        step //= 2
    return values


def offset_of(i):
    half = (i + 1) // 2
    return half * (2 * (i % 2) - 1) + NGY


def kernel(
    scalar_ref,
    vel_ref,
    out_ref,
    vel,
    packed,
    send_v,
    send_n,
    send_p,
    recv_v,
    recv_n,
    recv_p,
    hal_up,
    hal_dn,
    got_up,
    got_dn,
    refine,
    coarse,
    scal,
    fine,
    field,
    edge,
    shift,
    own,
    cross,
    part,
    recv_d,
    t_own,
    t_cross,
    send_o,
    send_c,
    recv_o,
    recv_c,
    joined,
    sems,
    column,
):
    gy, gz = lax.axis_index("gy"), lax.axis_index("gz")
    odd = gz % 2
    next_y, prev_y = (gy + 1) % NGY, (gy + NGY - 1) % NGY
    partner = gz + 1 - 2 * odd
    other = gz - 1 + 2 * odd
    has_other = jnp.logical_and(other >= 0, other < NGZ)
    lane = lax.broadcasted_iota(jnp.int32, (8, LANES), 1)

    take_vel = pltpu.make_async_copy(vel_ref, vel, sems.at[16])
    take_vel.start()
    for t in range(TILES):
        pltpu.make_async_copy(
            scalar_ref.at[:, :, LANES * t : LANES * t + LANES], scal.at[t], sems.at[17]
        ).start()

    barrier = pltpu.get_barrier_semaphore()

    def greet(y, z):
        pl.semaphore_signal(
            barrier, inc=1, device_id={"gy": y, "gz": z}, device_id_type=MESH
        )

    def greet_z(i, _):
        greet(gy, (gz + i) % NGZ)
        return _

    def greet_zn(i, _):
        greet(next_y, (gz + i) % NGZ)
        greet(prev_y, (gz + i) % NGZ)
        return _

    def greet_y(i, _):
        greet((gy + i) % NGY, gz)
        return _

    lax.fori_loop(0, NGZ, greet_zn, 0)
    lax.fori_loop(1, NGZ, greet_z, 0)
    lax.fori_loop(2, NGY - 1, greet_y, 0)

    @pl.when(jnp.logical_not(has_other))
    def _():
        joined[...] = jnp.zeros_like(joined)

    for block in range(16):
        r = lax.broadcasted_iota(jnp.int32, (16, NX), 0) + 16 * block
        c = lax.broadcasted_iota(jnp.int32, (16, NX), 1)
        t = jnp.abs(c - 3 * r)
        if block == 0:
            t = jnp.where(r == 0, jnp.minimum(t, jnp.abs(c - NX)), t)
        refine[16 * block : 16 * block + 16, :] = (
            jnp.maximum(3 - t, 0).astype(F32).astype(BF16)
        )

    take_vel.wait()
    for i in range(3):
        packed[8 + 64 * i : 72 + 64 * i, :] = vel[i].T
    for z in range(NGZ):
        send_v[z, 0:4, :] = packed[8 + 4 * z : 12 + 4 * z, :]
        send_v[z, 4:8, :] = packed[72 + 4 * z : 76 + 4 * z, :]
        up = packed[135 + 4 * z : 141 + 4 * z, :] if z < NGZ - 1 else packed[135 + 4 * z : 140 + 4 * z, :]
        if z == 0:
            row = lax.broadcasted_iota(jnp.int32, up.shape, 0)
            up = jnp.where(row == 0, 0.0, up)
        if z == NGZ - 1:
            send_v[z, 8:13, :] = up
            send_v[z, 13:14, :] = jnp.zeros((1, LANES), F32)
        else:
            send_v[z, 8:14, :] = up
    lane4 = lax.broadcasted_iota(jnp.int32, (4, LANES), 1)
    for z in range(NGZ):
        first = jnp.zeros((4, LANES), F32)
        last = jnp.zeros((4, LANES), F32)
        for q in range(4):
            if q < 3:
                rows = send_v[z, 4 * q : 4 * q + 4, :]
            else:
                rows = jnp.concatenate(
                    [send_v[z, 12:14, :], jnp.zeros((2, LANES), F32)], axis=0
                )
            here = jnp.logical_and(lane4 >= 32 * q, lane4 < 32 * q + 32)
            first = jnp.where(here, lane_roll(rows, 32 * q), first)
            if q < 2:
                last = jnp.where(here, lane_roll(rows, 32 + 32 * q), last)
        send_n[z] = first
        send_p[z] = last
    wait_for(scal, sems.at[17])
    for t in range(TILES):
        columns = pl.ds(LANES * t, LANES)
        for k in range(3):
            for z in range(PLANES):
                at = slice(4 * k + z, 4 * k + z + 1)
                hal_up[at, columns] = scal[t, z, k : k + 1, :]
                hal_dn[at, columns] = scal[t, z, 21 + k : 22 + k, :]

    pl.semaphore_wait(barrier, 76)

    @pl.when(has_other)
    def _():
        pl.semaphore_signal(
            column, inc=1, device_id={"gy": gy, "gz": other}, device_id_type=MESH
        )


    def send_z(i, _):
        z = (gz + offset_of(i)) % NGZ
        copy_to(send_v.at[z], recv_v.at[gz], sems.at[0], sems.at[1], gy, z).start()
        return _

    def send_zn(i, _):
        z = (gz + offset_of(i)) % NGZ
        copy_to(send_n.at[z], recv_n.at[gz], sems.at[2], sems.at[3], prev_y, z).start()
        copy_to(send_p.at[z], recv_p.at[gz], sems.at[4], sems.at[5], next_y, z).start()
        return _

    lax.fori_loop(1, NGZ, send_z, 0)
    lax.fori_loop(0, NGZ, send_zn, 0)
    to_prev = copy_to(hal_up, got_dn, sems.at[6], sems.at[7], prev_y, gz)
    to_next = copy_to(hal_dn, got_up, sems.at[8], sems.at[9], next_y, gz)
    to_prev.start()
    to_next.start()
    recv_v[gz] = send_v[gz]

    wait_for(recv_v.at[0:15], sems.at[1])
    wait_for(recv_n, sems.at[3])
    wait_for(recv_p, sems.at[5])

    for half in range(2):
        columns = pl.ds(LANES * half, LANES)
        for first, count in ((0, 8), (8, 6)):
            tiles = exchanged(
                [recv_v[8 * half + i, first : first + count, :] for i in range(8)],
                16,
                lane[0:count],
            )
            for c in range(8):
                base = 16 * (c + 2) + first
                coarse[base : base + count, columns] = tiles[c]
    for c in range(8):
        base = 16 * (c + 2) + 14
        coarse[base : base + 2, :] = jnp.zeros((2, 2 * LANES), F32)
    for source, first in ((recv_p, -2), (recv_n, 8)):
        tiles = exchanged(
            [jnp.concatenate([source[i], source[8 + i]], axis=0) for i in range(8)],
            16,
            lane,
        )
        for e in range(8):
            base = 16 * (first + e % 2 + 2) + 4 * (e // 2)
            coarse[base : base + 4, 0:LANES] = tiles[e][0:4]
            coarse[base : base + 4, LANES : 2 * LANES] = tiles[e][4:8]
    value = coarse[...]
    high = value.astype(BF16)
    low = (value - high.astype(F32)).astype(BF16)
    for pair in range(TILES // 2):
        weights = refine[:, 2 * LANES * pair : 2 * LANES * (pair + 1)]
        result = (
            jnp.dot(high, weights, preferred_element_type=F32)
            + jnp.dot(low, weights, preferred_element_type=F32)
        ) * (1.0 / 3.0)
        fine[2 * pair] = result[:, :LANES]
        fine[2 * pair + 1] = result[:, LANES:]

    def level(first, plane, t):
        return fine[t, pl.ds(16 * (first + 2) + plane, 8, stride=16), :]

    def edge_level(shift, plane, t):
        return jnp.concatenate(
            [
                fine[t, pl.ds(16 * (1 + shift) + plane, 4), :],
                fine[t, pl.ds(16 * (10 + shift) + plane, 4), :],
            ],
            axis=0,
        )

    def whole(load):
        return jnp.concatenate([load(t) for t in range(TILES)], axis=1)

    def spread(ref, rows, value):
        for t in range(TILES):
            ref[t, rows, :] = value[:, LANES * t : LANES * t + LANES]

    def mixed(base, following, k):
        return base if k == 0 else base * (1.0 - k / 3.0) + following * (k / 3.0)

    def shift_rows(group, k):
        return pl.ds(pl.multiple_of(ROWS * group + 8 * k, 8), 8)

    def shifts(group, base, following):
        for k in range(3):
            u = mixed(base, following, k)
            d = moved_by(u, lane_roll(u, 1), lane_roll(u, -1))
            spread(shift, shift_rows(group, k), d)

    def plane_shifts(z):
        shifts(z, whole(functools.partial(level, 0, z)), whole(functools.partial(level, 1, z)))

    def sweep_x(q, group, k, ref, rows):
        terms = products(q, whole(lambda t: shift[t, shift_rows(group, k), :]))
        total = terms[0]
        for m in (-3, -2, -1, 1, 2, 3):
            total = total + lane_roll(terms[m], m)
        spread(ref, rows, total)

    def plane_x(z):
        for k in range(3):
            q = whole(lambda t: scal[t, z, pl.ds(k, 8, stride=3), :])
            sweep_x(q, z, k, field, shift_rows(z, k))

    def step_x(z, _):
        plane_shifts(z + 1)
        plane_x(z)
        return _

    plane_shifts(0)
    lax.fori_loop(0, PLANES - 1, step_x, 0)
    shifts(
        PLANES,
        whole(functools.partial(edge_level, 0, 0)),
        whole(functools.partial(edge_level, 1, 0)),
    )
    plane_x(PLANES - 1)
    wait_for(got_up, sems.at[7])
    wait_for(got_dn, sems.at[9])
    for k in range(3):
        q = jnp.concatenate(
            [got_up[4 * k : 4 * k + 4, :], got_dn[4 * k : 4 * k + 4, :]], axis=0
        )
        sweep_x(q, PLANES, k, edge, slice(8 * k, 8 * k + 8))

    row = lax.broadcasted_iota(jnp.int32, (8, LANES), 0)

    def phases(before, base, following, q_of):
        u = [mixed(base, following, k) for k in range(3)]
        sides = [mixed(before, base, 2)] + u + [following]
        sums = {}
        for k in range(3):
            terms = products(q_of(k), moved_by(u[k], sides[k], sides[k + 2]))
            for m in range(-3, 4):
                key = ((k + m) % 3, (k + m) // 3)
                sums[key] = terms[m] if key not in sums else sums[key] + terms[m]
        return sums

    def tile_step(t, _):
        edges = phases(
            edge_level(-1, 4, t),
            edge_level(0, 4, t),
            edge_level(1, 4, t),
            lambda k: edge[t, 8 * k : 8 * k + 8, :],
        )
        swept = {}
        for z in range(PLANES):
            sums = phases(
                level(-1, 4 + z, t),
                level(0, 4 + z, t),
                level(1, 4 + z, t),
                lambda k: field[t, 8 * (3 * z + k) : 8 * (3 * z + k) + 8, :],
            )
            for k in range(3):
                above = jnp.where(
                    row == 0, row_roll(edges[k, 1], -z), row_roll(sums[k, 1], 1)
                )
                below = jnp.where(
                    row == 7, row_roll(edges[k, -1], 3 - z), row_roll(sums[k, -1], -1)
                )
                swept[z, k] = sums[k, 0] + above + below
        lower = [level(0, 8 + p, t) for p in range(6)]
        upper = [level(1, 8 + p, t) for p in range(6)]
        for k in range(3):
            u = [mixed(lower[p], upper[p], k) for p in range(6)]
            sums = {}
            for z in range(PLANES):
                terms = products(swept[z, k], moved_by(u[z + 1], u[z], u[z + 2]))
                for m in range(-3, 4):
                    sums[z + m] = terms[m] if z + m not in sums else sums[z + m] + terms[m]
            for z in range(PLANES):
                own[t, pl.ds(ROWS * z + k, 8, stride=3), :] = sums[z]
            for i in range(3):
                up, down = sums[4 + i], sums[i - 3]
                cross[t, pl.ds(ROWS * i + k, 8, stride=3), :] = jnp.where(
                    odd == 1, up, down
                )
                part[t, pl.ds(ROWS * i + k, 8, stride=3), :] = jnp.where(
                    odd == 1, down, up
                )
        return _

    def transposed(source, target, h):
        for i in range(TILES // 2):
            t = TILES // 2 * h + i
            rows = pl.ds(pl.multiple_of(LANES * t, LANES), LANES)
            target[rows, :] = source[t].T

    def rows_of(ref, y):
        base = ROWS * y
        return [
            ref[pl.ds(pl.multiple_of(base + 8 * i, 8), 8), :] for i in range(3)
        ]

    def in_groups(pack, send, h):
        def order(i):
            return NGY // 2 * h + (gy + offset_of((i + 1) % 16)) % (NGY // 2)

        for n in range(2):
            for i in range(8):
                pack(order(8 * n + i))
            if n:
                for i in range(8):
                    send(order(i))
        for i in range(8):
            send(order(i + 8))

    def pack_cross(y):
        v = rows_of(t_cross, y)
        send_c[y, 0:8, :] = jnp.where(lane < 72, v[0], lane_roll(v[2], 72))
        low = jnp.where(lane < 72, v[1], lane_roll(v[2], 16))
        low = jnp.where(lane < 88, low, row_roll(lane_roll(v[2], 32), -6))
        for q in range(3):
            piece = row_roll(lane_roll(v[1], 104 - 24 * q), 2 * q - 6)
            here = lane >= 104 if q == 0 else jnp.logical_and(lane >= 104, row >= 2 * q)
            low = jnp.where(here, piece, low)
        send_c[y, 8:14, :] = low[0:6]

    def send_cross(y):
        copy_to(
            send_c.at[y], recv_c.at[gy], sems.at[12], sems.at[13], y, other
        ).start()

    def pack_own(y):
        v = rows_of(t_own, y)
        end = lane_roll(v[2], 32)
        first = jnp.where(row >= 2, lane_roll(v[2], 96), row_roll(end, -2))
        second = jnp.where(row >= 2, lane_roll(v[2], 64), row_roll(end, -4))
        send_o[y, 0:8, :] = jnp.where(lane < 96, v[0], first)
        send_o[y, 8:16, :] = jnp.where(lane < 96, v[1], second)
        send_o[y, 16:18, :] = jnp.where(lane < 96, v[2], row_roll(end, -6))[0:2]

    def send_own(y):
        @pl.when(y != gy)
        def _():
            copy_to(
                send_o.at[y], recv_o.at[gy], sems.at[14], sems.at[15], y, gz
            ).start()

    def half_of(ref, h):
        return ref.at[pl.ds(TILES // 2 * h, TILES // 2)]

    def cross_step(step, carry):
        h = (gy + step) % 2

        def tiles(i, _):
            return tile_step(TILES // 2 * h + i, _)

        lax.fori_loop(0, TILES // 2, tiles, 0)
        copy_to(
            half_of(part, h), half_of(recv_d, h), sems.at[10], sems.at[18 + step], gy, partner
        ).start()

        @pl.when(has_other)
        def _():
            transposed(cross, t_cross, h)
            in_groups(pack_cross, send_cross, h)

        return carry

    @pl.when(has_other)
    def _():
        pl.semaphore_wait(column, 1)

    lax.fori_loop(0, 2, cross_step, 0)

    target = pl.ds(pl.multiple_of(ROWS * (1 - odd), 8), 72)

    def own_step(step, _):
        h = (gy + step) % 2
        wait_for(half_of(recv_d, h), sems.at[18 + step])
        tiles = pl.ds(TILES // 2 * h, TILES // 2)
        own[tiles, target, :] = own[tiles, target, :] + recv_d[tiles]
        transposed(own, t_own, h)
        in_groups(pack_own, send_own, h)
        return _

    lax.fori_loop(0, 2, own_step, 0)
    recv_o[gy] = send_o[gy]

    inside = lane - ROWS * odd
    keep = jnp.logical_and(inside >= 0, inside < 72)
    head = inside < 56

    @pl.when(has_other)
    def _():
        wait_for(recv_c, sems.at[13])

        turn = ROWS * odd

        def turned(value, amount):
            return pltpu.roll(value, (turn + amount) % LANES, 1)

        def open_cross(y, _):
            c0 = recv_c[y, 0:8, :]
            c1 = jnp.concatenate(
                [recv_c[y, 8:14, :], jnp.zeros((2, LANES), F32)], axis=0
            )
            tail = turned(row_roll(c1, 6), 24)
            for q in range(1, 3):
                piece = turned(row_roll(c1, 6 - 2 * q), 24 * q + 24)
                tail = jnp.where(inside < 24 * q, tail, piece)
            end = jnp.where(row < 6, turned(c1, 112), turned(row_roll(c1, 6), 96))
            e1 = jnp.where(row < 6, turned(c1, 0), tail)
            e2 = jnp.where(head, turned(c0, 56), end)
            joined[y, 0:8, :] = jnp.where(keep, turned(c0, 0), 0.0)
            joined[y, 8:16, :] = jnp.where(keep, e1, 0.0)
            joined[y, 16:24, :] = jnp.where(keep, e2, 0.0)
            return _

        lax.fori_loop(0, NGY, open_cross, 0, unroll=8)

    wait_for(recv_o.at[0 : NGY - 1], sems.at[15])

    def last_rows(y):
        p0, p1 = recv_o[y, 0:8, :], recv_o[y, 8:16, :]
        tail = recv_o[y, 16:18, :]
        tail = jnp.concatenate([tail, tail, tail, tail], axis=0)
        end = jnp.where(row < 6, row_roll(p1, 4), tail)
        end = lane_roll(jnp.where(row < 4, row_roll(p0, 2), end), 96)
        last = jnp.where(lane < 64, lane_roll(p1, 64), end)
        last = jnp.where(lane < 32, lane_roll(p0, 32), last)
        return jnp.where(row < 2, tail, last)

    for y in range(NGY):
        joined[y, 16:24, :] = joined[y, 16:24, :] + last_rows(y)
    for x in range(3):
        rows = slice(8 * x, 8 * x + 8)
        for t in range(TILES):
            pieces = [None] * PLANES
            for y in range(LANES * t // ROWS, (LANES * t + LANES - 1) // ROWS + 1):
                value = joined[y, rows, :]
                if x < 2:
                    value = value + recv_o[y, rows, :]
                edge_at = ROWS * y - LANES * t
                for z in range(PLANES):
                    turned_to = lane_roll(value, ROWS * (y - z))
                    pieces[z] = (
                        turned_to
                        if pieces[z] is None
                        else jnp.where(lane < edge_at, pieces[z], turned_to)
                    )
            for z in range(PLANES):
                out_ref[z, rows, LANES * t : LANES * t + LANES] = pieces[z]

    wait_for(send_v.at[0:15], sems.at[0])
    wait_for(send_n, sems.at[2])
    wait_for(send_p, sems.at[4])
    wait_for(hal_up, sems.at[6])
    wait_for(hal_dn, sems.at[8])
    wait_for(part, sems.at[10])
    wait_for(recv_o.at[0 : NGY - 1], sems.at[14])

    @pl.when(has_other)
    def _():
        wait_for(recv_c, sems.at[12])


def local(scalar, velocity):
    vmem = pl.BlockSpec(memory_space=pltpu.VMEM)
    buffers = [
        (3, LANES, 64),
        (208, LANES),
        (NGZ, 14, LANES),
        (NGZ, 4, LANES),
        (NGZ, 4, LANES),
        (NGZ, 14, LANES),
        (NGZ, 4, LANES),
        (NGZ, 4, LANES),
        (12, NX),
        (12, NX),
        (12, NX),
        (12, NX),
    ]
    later = [
        (192, 256),
        (TILES, PLANES, ROWS, LANES),
        (TILES, 192, LANES),
        (TILES, 96, LANES),
        (TILES, 24, LANES),
        (TILES, 120, LANES),
        (TILES, LANES, LANES),
        (TILES, LANES, LANES),
        (TILES, 72, LANES),
        (TILES, 72, LANES),
        (NX, LANES),
        (NX, LANES),
        (NGY, 18, LANES),
        (NGY, 14, LANES),
        (NGY, 18, LANES),
        (NGY, 14, LANES),
        (NGY, ROWS, LANES),
    ]
    return pl.pallas_call(
        kernel,
        out_shape=pltpu.VMEM((PLANES, ROWS, NX), F32),
        in_specs=[pl.BlockSpec(memory_space=pl.ANY)] * 2,
        out_specs=vmem,
        scratch_shapes=[pltpu.VMEM(s, F32) for s in buffers]
        + [pltpu.VMEM((256, NX), BF16)]
        + [pltpu.VMEM(s, F32) for s in later]
        + [pltpu.SemaphoreType.DMA((20,)), pltpu.SemaphoreType.REGULAR],
        compiler_params=pltpu.CompilerParams(collective_id=0, has_side_effects=True),
    )(scalar, velocity.transpose(0, 2, 3, 1).reshape(3, LANES, 64))


def solution(mesh):
    in_specs = (P("gz", "gy", None), P(None, None, "gy", "gz"))
    out_specs = P("gz", "gy", None)
    return jax.shard_map(
        local, mesh=mesh, in_specs=in_specs, out_specs=out_specs, check_vma=False
    )
```

```python
import functools

import jax
import jax.numpy as jnp
from jax import lax
from jax.experimental import pallas as pl
from jax.experimental.pallas import tpu as pltpu
from jax.sharding import PartitionSpec as P

MESH = pl.DeviceIdType.MESH
F32 = jnp.float32
BF16 = jnp.bfloat16
NGY = 32
NGZ = 16
PLANES = 4
ROWS = 24
NX = 768
LANES = 128
TILES = NX // LANES


def copy_to(src, dst, send, recv, gy, gz):
    return pltpu.make_async_remote_copy(
        src, dst, send, recv, device_id={"gy": gy, "gz": gz}, device_id_type=MESH
    )


def wait_for(ref, sem):
    pltpu.make_async_copy(ref, ref, sem).wait()


def moved_by(speed, before, after):
    half = jnp.abs(0.5 * speed)
    return speed + half * (jnp.where(speed >= 0.0, after, before) - speed)


def products(q, d):
    a = jnp.abs(d)
    d2 = d * d
    d3 = d2 * d
    s = (d3 - d) * (1.0 / 12.0)
    half = 0.5 * d
    r = s * half
    odd3 = d3 * ((1.0 - a) * (7.0 / 48.0 - (5.0 / 48.0) * a))
    even3 = jnp.abs(odd3)
    even2 = r - 6.0 * even3
    odd2 = s - 4.0 * odd3
    even1 = (0.5 * d2 - 4.0 * r) + 15.0 * even3
    odd1 = (half - 2.0 * s) + 5.0 * odd3
    middle = 1.0 - 2.0 * ((even1 + even2) + even3)
    return {
        0: q * middle,
        1: q * (even1 + odd1),
        -1: q * (even1 - odd1),
        2: q * (even2 + odd2),
        -2: q * (even2 - odd2),
        3: q * (even3 + odd3),
        -3: q * (even3 - odd3),
    }


def lane_roll(value, amount):
    amount = amount % value.shape[-1]
    return value if amount == 0 else pltpu.roll(value, amount, value.ndim - 1)


def row_roll(value, amount):
    amount = amount % value.shape[0]
    return value if amount == 0 else pltpu.roll(value, amount, 0)


def exchanged(values, width, lane):
    values = list(values)
    step = len(values) // 2
    while step:
        stay = jnp.zeros(lane.shape, jnp.bool_)
        for c in range(len(values)):
            if not c & step:
                stay = jnp.logical_or(
                    stay, jnp.logical_and(lane >= width * c, lane < width * (c + 1))
                )
        for i in range(len(values)):
            if not i & step:
                a, b = values[i], values[i + step]
                values[i] = jnp.where(stay, a, lane_roll(b, width * step))
                values[i + step] = jnp.where(stay, lane_roll(a, -width * step), b)
        step //= 2
    return values


def offset_of(i):
    half = (i + 1) // 2
    return half * (2 * (i % 2) - 1) + NGY


def kernel(
    scalar_ref,
    vel_ref,
    out_ref,
    vel,
    packed,
    send_v,
    send_n,
    send_p,
    recv_v,
    recv_n,
    recv_p,
    hal_up,
    hal_dn,
    got_up,
    got_dn,
    refine,
    coarse,
    scal,
    fine,
    field,
    edge,
    shift,
    own,
    cross,
    part,
    recv_d,
    t_own,
    t_cross,
    send_o,
    send_c,
    recv_o,
    recv_c,
    joined,
    sems,
    column,
):
    gy, gz = lax.axis_index("gy"), lax.axis_index("gz")
    odd = gz % 2
    next_y, prev_y = (gy + 1) % NGY, (gy + NGY - 1) % NGY
    partner = gz + 1 - 2 * odd
    other = gz - 1 + 2 * odd
    has_other = jnp.logical_and(other >= 0, other < NGZ)
    lane = lax.broadcasted_iota(jnp.int32, (8, LANES), 1)

    take_vel = pltpu.make_async_copy(vel_ref, vel, sems.at[16])
    take_vel.start()
    for t in range(TILES):
        pltpu.make_async_copy(
            scalar_ref.at[:, :, LANES * t : LANES * t + LANES], scal.at[t], sems.at[17]
        ).start()

    barrier = pltpu.get_barrier_semaphore()

    def greet(y, z):
        pl.semaphore_signal(
            barrier, inc=1, device_id={"gy": y, "gz": z}, device_id_type=MESH
        )

    def greet_z(i, _):
        greet(gy, (gz + i) % NGZ)
        return _

    def greet_zn(i, _):
        greet(next_y, (gz + i) % NGZ)
        greet(prev_y, (gz + i) % NGZ)
        return _

    def greet_y(i, _):
        greet((gy + i) % NGY, gz)
        return _

    lax.fori_loop(0, NGZ, greet_zn, 0)
    lax.fori_loop(1, NGZ, greet_z, 0)
    lax.fori_loop(2, NGY - 1, greet_y, 0)

    @pl.when(jnp.logical_not(has_other))
    def _():
        joined[...] = jnp.zeros_like(joined)

    for block in range(16):
        r = lax.broadcasted_iota(jnp.int32, (16, NX), 0) + 16 * block
        c = lax.broadcasted_iota(jnp.int32, (16, NX), 1)
        t = jnp.abs(c - 3 * r)
        if block == 0:
            t = jnp.where(r == 0, jnp.minimum(t, jnp.abs(c - NX)), t)
        refine[16 * block : 16 * block + 16, :] = (
            jnp.maximum(3 - t, 0).astype(F32).astype(BF16)
        )

    take_vel.wait()
    for i in range(3):
        packed[8 + 64 * i : 72 + 64 * i, :] = vel[i].T
    for z in range(NGZ):
        send_v[z, 0:4, :] = packed[8 + 4 * z : 12 + 4 * z, :]
        send_v[z, 4:8, :] = packed[72 + 4 * z : 76 + 4 * z, :]
        up = packed[135 + 4 * z : 141 + 4 * z, :] if z < NGZ - 1 else packed[135 + 4 * z : 140 + 4 * z, :]
        if z == 0:
            row = lax.broadcasted_iota(jnp.int32, up.shape, 0)
            up = jnp.where(row == 0, 0.0, up)
        if z == NGZ - 1:
            send_v[z, 8:13, :] = up
            send_v[z, 13:14, :] = jnp.zeros((1, LANES), F32)
        else:
            send_v[z, 8:14, :] = up
    lane4 = lax.broadcasted_iota(jnp.int32, (4, LANES), 1)
    for z in range(NGZ):
        first = jnp.zeros((4, LANES), F32)
        last = jnp.zeros((4, LANES), F32)
        for q in range(4):
            if q < 3:
                rows = send_v[z, 4 * q : 4 * q + 4, :]
            else:
                rows = jnp.concatenate(
                    [send_v[z, 12:14, :], jnp.zeros((2, LANES), F32)], axis=0
                )
            here = jnp.logical_and(lane4 >= 32 * q, lane4 < 32 * q + 32)
            first = jnp.where(here, lane_roll(rows, 32 * q), first)
            if q < 2:
                last = jnp.where(here, lane_roll(rows, 32 + 32 * q), last)
        send_n[z] = first
        send_p[z] = last
    wait_for(scal, sems.at[17])
    for t in range(TILES):
        columns = pl.ds(LANES * t, LANES)
        for k in range(3):
            for z in range(PLANES):
                at = slice(4 * k + z, 4 * k + z + 1)
                hal_up[at, columns] = scal[t, z, k : k + 1, :]
                hal_dn[at, columns] = scal[t, z, 21 + k : 22 + k, :]

    pl.semaphore_wait(barrier, 76)

    @pl.when(has_other)
    def _():
        pl.semaphore_signal(
            column, inc=1, device_id={"gy": gy, "gz": other}, device_id_type=MESH
        )


    def send_z(i, _):
        z = (gz + offset_of(i)) % NGZ
        copy_to(send_v.at[z], recv_v.at[gz], sems.at[0], sems.at[1], gy, z).start()
        return _

    def send_zn(i, _):
        z = (gz + offset_of(i)) % NGZ
        copy_to(send_n.at[z], recv_n.at[gz], sems.at[2], sems.at[3], prev_y, z).start()
        copy_to(send_p.at[z], recv_p.at[gz], sems.at[4], sems.at[5], next_y, z).start()
        return _

    lax.fori_loop(1, NGZ, send_z, 0)
    lax.fori_loop(0, NGZ, send_zn, 0)
    to_prev = copy_to(hal_up, got_dn, sems.at[6], sems.at[7], prev_y, gz)
    to_next = copy_to(hal_dn, got_up, sems.at[8], sems.at[9], next_y, gz)
    to_prev.start()
    to_next.start()
    recv_v[gz] = send_v[gz]

    wait_for(recv_v.at[0:15], sems.at[1])
    wait_for(recv_n, sems.at[3])
    wait_for(recv_p, sems.at[5])

    for half in range(2):
        columns = pl.ds(LANES * half, LANES)
        for first, count in ((0, 8), (8, 6)):
            tiles = exchanged(
                [recv_v[8 * half + i, first : first + count, :] for i in range(8)],
                16,
                lane[0:count],
            )
            for c in range(8):
                base = 16 * (c + 2) + first
                coarse[base : base + count, columns] = tiles[c]
    for c in range(8):
        base = 16 * (c + 2) + 14
        coarse[base : base + 2, :] = jnp.zeros((2, 2 * LANES), F32)
    for source, first in ((recv_p, -2), (recv_n, 8)):
        tiles = exchanged(
            [jnp.concatenate([source[i], source[8 + i]], axis=0) for i in range(8)],
            16,
            lane,
        )
        for e in range(8):
            base = 16 * (first + e % 2 + 2) + 4 * (e // 2)
            coarse[base : base + 4, 0:LANES] = tiles[e][0:4]
            coarse[base : base + 4, LANES : 2 * LANES] = tiles[e][4:8]
    value = coarse[...]
    high = value.astype(BF16)
    low = (value - high.astype(F32)).astype(BF16)
    for pair in range(TILES // 2):
        weights = refine[:, 2 * LANES * pair : 2 * LANES * (pair + 1)]
        result = (
            jnp.dot(high, weights, preferred_element_type=F32)
            + jnp.dot(low, weights, preferred_element_type=F32)
        ) * (1.0 / 3.0)
        fine[2 * pair] = result[:, :LANES]
        fine[2 * pair + 1] = result[:, LANES:]

    def level(first, plane, t):
        return fine[t, pl.ds(16 * (first + 2) + plane, 8, stride=16), :]

    def edge_level(shift, plane, t):
        return jnp.concatenate(
            [
                fine[t, pl.ds(16 * (1 + shift) + plane, 4), :],
                fine[t, pl.ds(16 * (10 + shift) + plane, 4), :],
            ],
            axis=0,
        )

    def whole(load):
        return jnp.concatenate([load(t) for t in range(TILES)], axis=1)

    def spread(ref, rows, value):
        for t in range(TILES):
            ref[t, rows, :] = value[:, LANES * t : LANES * t + LANES]

    def mixed(base, following, k):
        return base if k == 0 else base * (1.0 - k / 3.0) + following * (k / 3.0)

    def shift_rows(group, k):
        return pl.ds(pl.multiple_of(ROWS * group + 8 * k, 8), 8)

    def shifts(group, base, following):
        for k in range(3):
            u = mixed(base, following, k)
            d = moved_by(u, lane_roll(u, 1), lane_roll(u, -1))
            spread(shift, shift_rows(group, k), d)

    def plane_shifts(z):
        shifts(z, whole(functools.partial(level, 0, z)), whole(functools.partial(level, 1, z)))

    def sweep_x(q, group, k, ref, rows):
        terms = products(q, whole(lambda t: shift[t, shift_rows(group, k), :]))
        total = terms[0]
        for m in (-3, -2, -1, 1, 2, 3):
            total = total + lane_roll(terms[m], m)
        spread(ref, rows, total)

    def plane_x(z):
        for k in range(3):
            q = whole(lambda t: scal[t, z, pl.ds(k, 8, stride=3), :])
            sweep_x(q, z, k, field, shift_rows(z, k))

    def step_x(z, _):
        plane_shifts(z + 1)
        plane_x(z)
        return _

    plane_shifts(0)
    lax.fori_loop(0, PLANES - 1, step_x, 0)
    shifts(
        PLANES,
        whole(functools.partial(edge_level, 0, 0)),
        whole(functools.partial(edge_level, 1, 0)),
    )
    plane_x(PLANES - 1)
    wait_for(got_up, sems.at[7])
    wait_for(got_dn, sems.at[9])
    for k in range(3):
        q = jnp.concatenate(
            [got_up[4 * k : 4 * k + 4, :], got_dn[4 * k : 4 * k + 4, :]], axis=0
        )
        sweep_x(q, PLANES, k, edge, slice(8 * k, 8 * k + 8))

    row = lax.broadcasted_iota(jnp.int32, (8, LANES), 0)

    def phases(before, base, following, q_of):
        u = [mixed(base, following, k) for k in range(3)]
        sides = [mixed(before, base, 2)] + u + [following]
        sums = {}
        for k in range(3):
            terms = products(q_of(k), moved_by(u[k], sides[k], sides[k + 2]))
            for m in range(-3, 4):
                key = ((k + m) % 3, (k + m) // 3)
                sums[key] = terms[m] if key not in sums else sums[key] + terms[m]
        return sums

    def tile_step(t, _):
        edges = phases(
            edge_level(-1, 4, t),
            edge_level(0, 4, t),
            edge_level(1, 4, t),
            lambda k: edge[t, 8 * k : 8 * k + 8, :],
        )
        swept = {}
        for z in range(PLANES):
            sums = phases(
                level(-1, 4 + z, t),
                level(0, 4 + z, t),
                level(1, 4 + z, t),
                lambda k: field[t, 8 * (3 * z + k) : 8 * (3 * z + k) + 8, :],
            )
            for k in range(3):
                above = jnp.where(
                    row == 0, row_roll(edges[k, 1], -z), row_roll(sums[k, 1], 1)
                )
                below = jnp.where(
                    row == 7, row_roll(edges[k, -1], 3 - z), row_roll(sums[k, -1], -1)
                )
                swept[z, k] = sums[k, 0] + above + below
        lower = [level(0, 8 + p, t) for p in range(6)]
        upper = [level(1, 8 + p, t) for p in range(6)]
        for k in range(3):
            u = [mixed(lower[p], upper[p], k) for p in range(6)]
            sums = {}
            for z in range(PLANES):
                terms = products(swept[z, k], moved_by(u[z + 1], u[z], u[z + 2]))
                for m in range(-3, 4):
                    sums[z + m] = terms[m] if z + m not in sums else sums[z + m] + terms[m]
            for z in range(PLANES):
                own[t, pl.ds(ROWS * z + k, 8, stride=3), :] = sums[z]
            for i in range(3):
                up, down = sums[4 + i], sums[i - 3]
                cross[t, pl.ds(ROWS * i + k, 8, stride=3), :] = jnp.where(
                    odd == 1, up, down
                )
                part[t, pl.ds(ROWS * i + k, 8, stride=3), :] = jnp.where(
                    odd == 1, down, up
                )
        return _

    def transposed(source, target, h):
        for i in range(TILES // 2):
            t = TILES // 2 * h + i
            rows = pl.ds(pl.multiple_of(LANES * t, LANES), LANES)
            target[rows, :] = source[t].T

    def rows_of(ref, y):
        base = ROWS * y
        return [
            ref[pl.ds(pl.multiple_of(base + 8 * i, 8), 8), :] for i in range(3)
        ]

    def in_groups(pack, send, h):
        def order(i):
            return NGY // 2 * h + (gy + offset_of((i + 1) % 16)) % (NGY // 2)

        for n in range(2):
            for i in range(8):
                pack(order(8 * n + i))
            if n:
                for i in range(8):
                    send(order(i))
        for i in range(8):
            send(order(i + 8))

    def pack_cross(y):
        v = rows_of(t_cross, y)
        send_c[y, 0:8, :] = jnp.where(lane < 72, v[0], lane_roll(v[2], 72))
        low = jnp.where(lane < 72, v[1], lane_roll(v[2], 16))
        low = jnp.where(lane < 88, low, row_roll(lane_roll(v[2], 32), -6))
        for q in range(3):
            piece = row_roll(lane_roll(v[1], 104 - 24 * q), 2 * q - 6)
            here = lane >= 104 if q == 0 else jnp.logical_and(lane >= 104, row >= 2 * q)
            low = jnp.where(here, piece, low)
        send_c[y, 8:14, :] = low[0:6]

    def send_cross(y):
        copy_to(
            send_c.at[y], recv_c.at[gy], sems.at[12], sems.at[13], y, other
        ).start()

    def pack_own(y):
        v = rows_of(t_own, y)
        end = lane_roll(v[2], 32)
        first = jnp.where(row >= 2, lane_roll(v[2], 96), row_roll(end, -2))
        second = jnp.where(row >= 2, lane_roll(v[2], 64), row_roll(end, -4))
        send_o[y, 0:8, :] = jnp.where(lane < 96, v[0], first)
        send_o[y, 8:16, :] = jnp.where(lane < 96, v[1], second)
        send_o[y, 16:18, :] = jnp.where(lane < 96, v[2], row_roll(end, -6))[0:2]

    def send_own(y):
        @pl.when(y != gy)
        def _():
            copy_to(
                send_o.at[y], recv_o.at[gy], sems.at[14], sems.at[15], y, gz
            ).start()

    def half_of(ref, h):
        return ref.at[pl.ds(TILES // 2 * h, TILES // 2)]

    def cross_step(step, carry):
        h = (gy // 4 + step) % 2

        def tiles(i, _):
            return tile_step(TILES // 2 * h + i, _)

        lax.fori_loop(0, TILES // 2, tiles, 0)
        copy_to(
            half_of(part, h), half_of(recv_d, h), sems.at[10], sems.at[18 + step], gy, partner
        ).start()

        @pl.when(has_other)
        def _():
            transposed(cross, t_cross, h)
            in_groups(pack_cross, send_cross, h)

        return carry

    @pl.when(has_other)
    def _():
        pl.semaphore_wait(column, 1)

    lax.fori_loop(0, 2, cross_step, 0)

    target = pl.ds(pl.multiple_of(ROWS * (1 - odd), 8), 72)

    def own_step(step, _):
        h = (gy // 4 + step) % 2
        wait_for(half_of(recv_d, h), sems.at[18 + step])
        tiles = pl.ds(TILES // 2 * h, TILES // 2)
        own[tiles, target, :] = own[tiles, target, :] + recv_d[tiles]
        transposed(own, t_own, h)
        in_groups(pack_own, send_own, h)
        return _

    lax.fori_loop(0, 2, own_step, 0)
    recv_o[gy] = send_o[gy]

    inside = lane - ROWS * odd
    keep = jnp.logical_and(inside >= 0, inside < 72)
    head = inside < 56

    @pl.when(has_other)
    def _():
        wait_for(recv_c, sems.at[13])

        turn = ROWS * odd

        def turned(value, amount):
            return pltpu.roll(value, (turn + amount) % LANES, 1)

        def open_cross(y, _):
            c0 = recv_c[y, 0:8, :]
            c1 = jnp.concatenate(
                [recv_c[y, 8:14, :], jnp.zeros((2, LANES), F32)], axis=0
            )
            tail = turned(row_roll(c1, 6), 24)
            for q in range(1, 3):
                piece = turned(row_roll(c1, 6 - 2 * q), 24 * q + 24)
                tail = jnp.where(inside < 24 * q, tail, piece)
            end = jnp.where(row < 6, turned(c1, 112), turned(row_roll(c1, 6), 96))
            e1 = jnp.where(row < 6, turned(c1, 0), tail)
            e2 = jnp.where(head, turned(c0, 56), end)
            joined[y, 0:8, :] = jnp.where(keep, turned(c0, 0), 0.0)
            joined[y, 8:16, :] = jnp.where(keep, e1, 0.0)
            joined[y, 16:24, :] = jnp.where(keep, e2, 0.0)
            return _

        lax.fori_loop(0, NGY, open_cross, 0, unroll=8)

    wait_for(recv_o.at[0 : NGY - 1], sems.at[15])

    def last_rows(y):
        p0, p1 = recv_o[y, 0:8, :], recv_o[y, 8:16, :]
        tail = recv_o[y, 16:18, :]
        tail = jnp.concatenate([tail, tail, tail, tail], axis=0)
        end = jnp.where(row < 6, row_roll(p1, 4), tail)
        end = lane_roll(jnp.where(row < 4, row_roll(p0, 2), end), 96)
        last = jnp.where(lane < 64, lane_roll(p1, 64), end)
        last = jnp.where(lane < 32, lane_roll(p0, 32), last)
        return jnp.where(row < 2, tail, last)

    for y in range(NGY):
        joined[y, 16:24, :] = joined[y, 16:24, :] + last_rows(y)
    for x in range(3):
        rows = slice(8 * x, 8 * x + 8)
        for t in range(TILES):
            pieces = [None] * PLANES
            for y in range(LANES * t // ROWS, (LANES * t + LANES - 1) // ROWS + 1):
                value = joined[y, rows, :]
                if x < 2:
                    value = value + recv_o[y, rows, :]
                edge_at = ROWS * y - LANES * t
                for z in range(PLANES):
                    turned_to = lane_roll(value, ROWS * (y - z))
                    pieces[z] = (
                        turned_to
                        if pieces[z] is None
                        else jnp.where(lane < edge_at, pieces[z], turned_to)
                    )
            for z in range(PLANES):
                out_ref[z, rows, LANES * t : LANES * t + LANES] = pieces[z]

    wait_for(send_v.at[0:15], sems.at[0])
    wait_for(send_n, sems.at[2])
    wait_for(send_p, sems.at[4])
    wait_for(hal_up, sems.at[6])
    wait_for(hal_dn, sems.at[8])
    wait_for(part, sems.at[10])
    wait_for(recv_o.at[0 : NGY - 1], sems.at[14])

    @pl.when(has_other)
    def _():
        wait_for(recv_c, sems.at[12])


def local(scalar, velocity):
    vmem = pl.BlockSpec(memory_space=pltpu.VMEM)
    buffers = [
        (3, LANES, 64),
        (208, LANES),
        (NGZ, 14, LANES),
        (NGZ, 4, LANES),
        (NGZ, 4, LANES),
        (NGZ, 14, LANES),
        (NGZ, 4, LANES),
        (NGZ, 4, LANES),
        (12, NX),
        (12, NX),
        (12, NX),
        (12, NX),
    ]
    later = [
        (192, 256),
        (TILES, PLANES, ROWS, LANES),
        (TILES, 192, LANES),
        (TILES, 96, LANES),
        (TILES, 24, LANES),
        (TILES, 120, LANES),
        (TILES, LANES, LANES),
        (TILES, LANES, LANES),
        (TILES, 72, LANES),
        (TILES, 72, LANES),
        (NX, LANES),
        (NX, LANES),
        (NGY, 18, LANES),
        (NGY, 14, LANES),
        (NGY, 18, LANES),
        (NGY, 14, LANES),
        (NGY, ROWS, LANES),
    ]
    return pl.pallas_call(
        kernel,
        out_shape=pltpu.VMEM((PLANES, ROWS, NX), F32),
        in_specs=[pl.BlockSpec(memory_space=pl.ANY)] * 2,
        out_specs=vmem,
        scratch_shapes=[pltpu.VMEM(s, F32) for s in buffers]
        + [pltpu.VMEM((256, NX), BF16)]
        + [pltpu.VMEM(s, F32) for s in later]
        + [pltpu.SemaphoreType.DMA((20,)), pltpu.SemaphoreType.REGULAR],
        compiler_params=pltpu.CompilerParams(collective_id=0, has_side_effects=True),
    )(scalar, velocity.transpose(0, 2, 3, 1).reshape(3, LANES, 64))


def solution(mesh):
    in_specs = (P("gz", "gy", None), P(None, None, "gy", "gz"))
    out_specs = P("gz", "gy", None)
    return jax.shard_map(
        local, mesh=mesh, in_specs=in_specs, out_specs=out_specs, check_vma=False
    )
```
